128 devices in a mesh: mem: 32 (over z, y, core), emb: 4 (over x).
Axes of the slice: x: 4, y: 4, z: 4, core: 2. Of those that a mesh axis runs over, the one named last changes fastest.
Arguments:
- memory: float32 [131072, 512], P('mem', 'emb'), may hold values from -6 to 6
- ev_rows: int32 [32, 32, 32], P('mem'), may hold values from 0 to 4095, as said below
- ev_count: int32 [32, 32], P('mem'), may hold values from 4 to 32, as said below
- ev_feat: bfloat16 [32, 32, 32, 128], P('mem'), may hold values from -6 to 6
- ev_dt: int32 [32, 32, 32], P('mem'), may hold values from 0 to 1000
- req_rows: int32 [32, 32, 528], P('mem'), may hold values from 0 to 4095, as said below
- nbr_slot: int32 [8192, 33], P('mem'), may hold values from 0 to 16895, as said below
- nbr_dt: int32 [8192, 33], P(('mem', 'emb')), may hold values from 0 to 1000
- nbr_len: int32 [8192], P(('mem', 'emb')), may hold values from 1 to 32
- time_freq: float32 [128], replicated, may hold values from 0.001 to 1
- gru_wx: bfloat16 [3, 256, 512], P(None, None, 'emb'), may hold values from -0.375 to 0.375
- gru_wh: bfloat16 [3, 512, 512], P(None, None, 'emb'), may hold values from -0.25 to 0.25
- gru_bias: float32 [4, 512], P(None, 'emb'), may hold values from -3 to 3
- w_query: bfloat16 [512, 512], replicated, may hold values from -0.25 to 0.25
- w_key: bfloat16 [512, 512], replicated, may hold values from -0.25 to 0.25
- w_value: bfloat16 [512, 512], replicated, may hold values from -0.25 to 0.25
- w_time: bfloat16 [128, 512], replicated, may hold values from -0.5 to 0.5
- w_out: bfloat16 [512, 512], replicated, may hold values from -0.25 to 0.25
- cotangent: bfloat16 [8192, 512], P(('mem', 'emb')), may hold values from -0.119628906 to 0.119628906
Outputs:
- new_memory: float32 [131072, 512], P('mem', 'emb')
- embeddings: bfloat16 [8192, 512], P(('mem', 'emb'))
- grad_wx: float32 [3, 256, 512], P(None, None, 'emb')
- grad_wh: float32 [3, 512, 512], P(None, None, 'emb')
- grad_bias: float32 [4, 512], P(None, 'emb')
- grad_query: float32 [512, 512], replicated
- grad_key: float32 [512, 512], replicated
- grad_value: float32 [512, 512], replicated
- grad_time: float32 [128, 512], replicated
- grad_out: float32 [512, 512], replicated
The draws below stay inside these ranges and needn't reach their ends.
Inputs may be any that keep to these rules, and one draw needn't show every extreme that they name: `ev_rows`: owner o holds rows o * 4096 to (o + 1) * 4096 - 1. All 1024 slots bound for one owner, live or not, name distinct rows. Slots [s, o, i] with i < ev_count[s, o] are live, the others padding. In every draw some owner receives all 32 slots live from every sender group. `req_rows`: rows may repeat. Only slots that nbr_slot refers to are read. `nbr_slot`: entry [b, j] is o * 528 + i, a slot of bucket [b // 256, o] of req_rows. In every group the referenced slots of each bucket lie among its first so many, and in every draw some owner's bucket may be referenced up to slot 527 in every group.
All inputs are finite; a program needn't handle non-finite values.
Results may differ from the reference program's by a relative error of at most 0.012.
Values may be sent and summed in bfloat16 or wider, within the bound.
No kernel may reach another device: no remote copies, remote signals or barrier semaphores. Data moves between devices by JAX's collectives and lax.ppermute only.
A program may use at most 128 MiB of HBM per device.

```python
import math
import jax
import jax.numpy as jnp
from jax import lax

W = 512
EF = 128
TE = 128
HEADS = 2
K = 32
SLOT = 32
ROWS_DEV = 4096
B_DEV = 256
MSG = 256
RCAP = 528
NODES = 131072
B_TOTAL = 8192
N_MEM = 32


def bucket_fill(key, salt, capacity):
    hot_owner = jax.random.randint(jax.random.fold_in(key, salt), (), 0, N_MEM)
    filled = jax.random.randint(jax.random.fold_in(key, salt + 1), (N_MEM, N_MEM), capacity // 8, 3 * capacity // 4 + 1)
    owner_ids = jnp.arange(N_MEM, dtype=jnp.int32)[None, :]
    return jnp.where(owner_ids == hot_owner, capacity, filled).astype(jnp.int32)


def draw_ev_count(key, part):
    return bucket_fill(key, 101, SLOT)


def draw_ev_rows(key, part):
    key_list = jax.random.split(jax.random.fold_in(key, 202), N_MEM)

    def one_owner(owner_key):
        return jax.random.permutation(owner_key, ROWS_DEV)[:N_MEM * SLOT].reshape(N_MEM, SLOT)
    layout = jax.vmap(one_owner)(key_list)
    return jnp.transpose(layout, (1, 0, 2)).astype(jnp.int32)


def draw_req_rows(key, part):
    return jax.random.randint(jax.random.fold_in(key, 303), (N_MEM, N_MEM, RCAP), 0, ROWS_DEV).astype(jnp.int32)


def draw_nbr_slot(key, part):
    filled = bucket_fill(key, 404, RCAP)
    totals = jnp.sum(filled, axis=1)
    endings = jnp.cumsum(filled, axis=1)
    starting = endings - filled
    group_ids = jnp.arange(B_DEV * N_MEM, dtype=jnp.int32) // B_DEV
    raw_picks = jax.random.randint(jax.random.fold_in(key, 505), (B_DEV * N_MEM, K + 1), 0, 2 ** 30)
    picks = raw_picks % totals[group_ids][:, None]
    owner_ids = jnp.sum((picks[:, :, None] >= endings[group_ids][:, None, :]).astype(jnp.int32), axis=-1)
    offsets = jnp.take_along_axis(starting[group_ids], owner_ids, axis=1)
    return (owner_ids * RCAP + picks - offsets).astype(jnp.int32)


def touch_ends(entries, stream_key, low, largest):
    longest = entries.shape.index(max(entries.shape))
    spots = []
    for shift in (0, 1):
        where = [jax.random.randint(jax.random.fold_in(stream_key, axis), (), 0, length) for axis, length in enumerate(entries.shape)]
        where[longest] = (where[longest] + shift) % entries.shape[longest]
        spots.append(tuple(where))
    return entries.at[spots[0]].set(low).at[spots[1]].set(largest)


def shard_levels(key, shape, shards, least, top_value):
    def one(axis_at, shards_of):
        heights = jax.random.uniform(jax.random.fold_in(jax.random.fold_in(key, 6), axis_at), (shards_of,), jnp.float32, least / len(shards), top_value / len(shards))
        return jnp.repeat(jnp.exp(heights), shape[axis_at] // shards_of).reshape((-1,) + (1,) * (len(shape) - axis_at - 1))

    level = one(*shards[0])
    for cut in shards[1:]:
        level = level * one(*cut)
    return level


def centred(rng, extent, scale, limit, cuts=(), held_as=jnp.bfloat16):
    array = jax.random.normal(rng, extent, jnp.float32) * scale
    if len(cuts) > 0:
        array = shard_levels(rng, extent, cuts, -0.22, 0.18) * array
    return jnp.clip(array, min=-limit, max=limit).astype(held_as)


def setup_inputs(seed: int = 0) -> dict:
    splits = jax.random.split(jax.random.key(seed), 20)
    return {
        "memory": centred(splits[0], (NODES, W), 1.0, 6.0, ((0, 32), (1, 4)), jnp.float32),
        "ev_rows": draw_ev_rows(jax.random.fold_in(splits[19], 71), 0),
        "ev_count": draw_ev_count(jax.random.fold_in(splits[19], 71), 0),
        "ev_feat": centred(splits[3], (N_MEM, N_MEM, SLOT, EF), 1.0, 6.0, ((0, 32),)),
        "ev_dt": touch_ends(jax.random.randint(splits[4], (N_MEM, N_MEM, SLOT), 0, 1001), jax.random.fold_in(splits[4], 1), 0, 1000).astype(jnp.int32),
        "req_rows": draw_req_rows(jax.random.fold_in(splits[19], 71), 0),
        "nbr_slot": draw_nbr_slot(jax.random.fold_in(splits[19], 71), 0),
        "nbr_dt": touch_ends(jax.random.randint(splits[7], (B_TOTAL, K + 1), 0, 1001), jax.random.fold_in(splits[7], 1), 0, 1000).astype(jnp.int32),
        "nbr_len": touch_ends(jax.random.randint(splits[8], (B_TOTAL,), 1, K + 1), jax.random.fold_in(splits[8], 1), 1, K).astype(jnp.int32),
        "time_freq": jnp.clip(jnp.exp(jax.random.uniform(splits[9], (TE,), jnp.float32, math.log(0.001), math.log(1.0))), 0.001, 1.0),
        "gru_wx": centred(splits[10], (3, MSG, W), MSG ** -0.5, 0.375, ((2, 4),)),
        "gru_wh": centred(splits[11], (3, W, W), W ** -0.5, 0.25, ((2, 4),)),
        "gru_bias": centred(splits[12], (4, W), 0.5, 3.0, ((1, 4),), jnp.float32),
        "w_query": centred(splits[13], (W, W), W ** -0.5, 0.25),
        "w_key": centred(splits[14], (W, W), W ** -0.5, 0.25),
        "w_value": centred(splits[15], (W, W), W ** -0.5, 0.25),
        "w_time": centred(splits[16], (TE, W), TE ** -0.5, 0.5),
        "w_out": centred(splits[17], (W, W), W ** -0.5, 0.25),
        "cotangent": centred(splits[18], (B_TOTAL, W), 0.02, 0.119628906, ((0, 128),)),
    }


EPSILON = 1e-06

def matmul(left_side, right_side):
    return jnp.dot(left_side, right_side, preferred_element_type=jnp.float32)

def matmul_left(left_side, right_side):
    return lax.dot_general(left_side, right_side, (((0,), (0,)), ((), ())), preferred_element_type=jnp.float32)

def matmul_right(left_side, right_side):
    return lax.dot_general(left_side, right_side, (((1,), (1,)), ((), ())), preferred_element_type=jnp.float32)

def time_code(time_delta, time_freq):
    return jnp.cos(time_delta.astype(jnp.float32)[..., None] * time_freq).astype(jnp.bfloat16)

def gru_forward(inputs, hidden_wide, stale_rows, gru_wx, gru_wh, gru_bias):
    reset_gate = jax.nn.sigmoid(matmul(inputs, gru_wx[0]) + matmul(hidden_wide, gru_wh[0]) + gru_bias[0])
    update = jax.nn.sigmoid(matmul(inputs, gru_wx[1]) + matmul(hidden_wide, gru_wh[1]) + gru_bias[1])
    recall = matmul(hidden_wide, gru_wh[2]) + gru_bias[3]
    candidate = jnp.tanh(matmul(inputs, gru_wx[2]) + gru_bias[2] + reset_gate * recall)
    fresh_rows = (1.0 - update) * candidate + update * stale_rows
    return (fresh_rows, (reset_gate, update, recall, candidate))

def gru_backward(grad_rows, inputs, hidden_wide, stale_rows, gate_state):
    reset_gate, update, recall, candidate = gate_state
    cand_term = grad_rows * (1.0 - update) * (1.0 - candidate * candidate)
    update_term = grad_rows * (stale_rows - candidate) * update * (1.0 - update)
    recall_term = cand_term * reset_gate
    reset_term = cand_term * recall * reset_gate * (1.0 - reset_gate)
    grad_terms = [reset_term, update_term, cand_term, recall_term]
    rounded = [member.astype(jnp.bfloat16) for member in grad_terms]
    grad_wx = jnp.stack([matmul_left(inputs, rounded[0]), matmul_left(inputs, rounded[1]), matmul_left(inputs, rounded[2])])
    grad_wh = jnp.stack([matmul_left(hidden_wide, rounded[0]), matmul_left(hidden_wide, rounded[1]), matmul_left(hidden_wide, rounded[3])])
    grad_bias = jnp.stack([lax.optimization_barrier(jnp.sum(member, axis=0)) for member in grad_terms])
    return (grad_wx, grad_wh, grad_bias)

def attend_core(queries, key_rows, values, valid_mask):
    node_count, model_width = queries.shape
    key_count = key_rows.shape[1]
    head_width = model_width // HEADS
    query_heads = queries.reshape(node_count, HEADS, head_width)
    key_heads = key_rows.reshape(node_count, key_count, HEADS, head_width)
    value_heads = values.reshape(node_count, key_count, HEADS, head_width)
    query_heads = query_heads * lax.rsqrt(lax.optimization_barrier(jnp.mean(query_heads * query_heads, axis=-1, keepdims=True)) + EPSILON)
    key_heads = key_heads * lax.rsqrt(lax.optimization_barrier(jnp.mean(key_heads * key_heads, axis=-1, keepdims=True)) + EPSILON)
    scores = jnp.einsum('nhd,njhd->nhj', query_heads, key_heads, precision=lax.Precision.HIGHEST) / math.sqrt(head_width)
    weights = jnp.exp(scores) * valid_mask[:, None, :]
    weights = weights / lax.optimization_barrier(jnp.sum(weights, axis=-1, keepdims=True))
    mixed = jnp.einsum('nhj,njhd->nhd', weights, value_heads, precision=lax.Precision.HIGHEST)
    return mixed.reshape(node_count, model_width)

def attend(node_rows, time_delta, lengths, time_freq, w_query, w_key, w_value, w_time, w_out, cotangent):
    node_count, key_count, model_width = node_rows.shape
    self_rows = node_rows[:, 0]
    time_codes = time_code(time_delta, time_freq)
    flat_rows = node_rows.reshape(node_count * key_count, model_width)
    flat_code = time_codes.reshape(node_count * key_count, time_codes.shape[-1])
    queries = matmul(self_rows, w_query).astype(jnp.bfloat16)
    key_rows = (matmul(flat_rows, w_key) + matmul(flat_code, w_time)).astype(jnp.bfloat16)
    values = matmul(flat_rows, w_value).astype(jnp.bfloat16)
    valid_mask = (jnp.arange(key_count, dtype=jnp.int32)[None, :] <= lengths[:, None]).astype(jnp.float32)

    def core(query_in, key_in, value_in):
        return attend_core(query_in, key_in.reshape(node_count, key_count, model_width), value_in.reshape(node_count, key_count, model_width), valid_mask)
    mixed, pullback = jax.vjp(core, queries.astype(jnp.float32), key_rows.astype(jnp.float32), values.astype(jnp.float32))
    mixed_half = mixed.astype(jnp.bfloat16)
    embedding = (matmul(mixed_half, w_out) + self_rows.astype(jnp.float32)).astype(jnp.bfloat16)
    grad_out = matmul_left(mixed_half, cotangent)
    query_grad, key_grad, value_grad = [member.astype(jnp.bfloat16) for member in pullback(matmul_right(cotangent, w_out))]
    grad_query = matmul_left(self_rows, query_grad)
    grad_key = matmul_left(flat_rows, key_grad)
    grad_time = matmul_left(flat_code, key_grad)
    grad_value = matmul_left(flat_rows, value_grad)
    rows_grad = (matmul_right(key_grad, w_key) + matmul_right(value_grad, w_value)).reshape(node_count, key_count, model_width)
    self_grad = matmul_right(query_grad, w_query) + cotangent.astype(jnp.float32)
    rows_grad = rows_grad.at[:, 0].add(self_grad).astype(jnp.bfloat16)
    return (embedding, (grad_query, grad_key, grad_value, grad_time, grad_out), rows_grad)

def reference(memory, ev_rows, ev_count, ev_feat, ev_dt, req_rows, nbr_slot, nbr_dt, nbr_len, time_freq, gru_wx, gru_wh, gru_bias, w_query, w_key, w_value, w_time, w_out, cotangent):
    groups = ev_rows.shape[0]
    slot_count = ev_rows.shape[2]
    model_width = memory.shape[1]
    rows_dev = memory.shape[0] // groups
    capacity = req_rows.shape[2]
    batch_dev = nbr_slot.shape[0] // groups
    key_count = nbr_slot.shape[1]
    message = jnp.concatenate([ev_feat, time_code(ev_dt, time_freq)], axis=-1)
    message = message.reshape(-1, message.shape[-1])
    owner_base = jnp.arange(groups, dtype=jnp.int32)[None, :, None] * rows_dev
    target = (owner_base + ev_rows).reshape(-1)
    live_mask = (jnp.arange(slot_count, dtype=jnp.int32)[None, None, :] < ev_count[:, :, None]).reshape(-1)
    stale_rows = memory[target]
    hidden_wide = stale_rows.astype(jnp.bfloat16)
    fresh_rows, gate_state = gru_forward(message, hidden_wide, stale_rows, gru_wx, gru_wh, gru_bias)
    new_memory = memory.at[target].set(jnp.where(live_mask[:, None], fresh_rows, stale_rows))
    group_ids = jnp.arange(groups * batch_dev, dtype=jnp.int32) // batch_dev
    owner_ids = nbr_slot // capacity
    local_ids = req_rows[group_ids[:, None], owner_ids, nbr_slot % capacity]
    node_ids = owner_ids * rows_dev + local_ids

    def one_group(blocks):
        id_block, delta_block, length_block, cot_block = blocks
        node_rows = new_memory[id_block].astype(jnp.bfloat16)
        return attend(node_rows, delta_block, length_block, time_freq, w_query, w_key, w_value, w_time, w_out, cot_block)
    embedding, weight_grads, rows_grad = lax.map(one_group, (node_ids.reshape(groups, batch_dev, key_count), nbr_dt.reshape(groups, batch_dev, key_count), nbr_len.reshape(groups, batch_dev), cotangent.reshape(groups, batch_dev, model_width)))
    embeddings = embedding.reshape(-1, model_width)
    weight_grads = tuple((lax.optimization_barrier(jnp.sum(member, axis=0)) for member in weight_grads))
    owner_rows = jnp.arange(groups, dtype=jnp.int32)[:, None] * rows_dev

    def add_group(total, blocks):
        slot_block, grad_block, asked_block = blocks
        sums = jnp.zeros((groups * capacity, model_width), jnp.float32).at[slot_block].add(grad_block.astype(jnp.float32))
        sums = lax.optimization_barrier(sums.astype(jnp.bfloat16)).astype(jnp.float32)
        rows_of = (owner_rows + asked_block).reshape(-1)
        return (total.at[rows_of].add(sums), None)
    memory_grad, _ = lax.scan(add_group, jnp.zeros_like(memory), (nbr_slot.reshape(groups, batch_dev * key_count), rows_grad.reshape(groups, batch_dev * key_count, model_width), req_rows))
    grad_fresh = jnp.where(live_mask[:, None], memory_grad[target], 0.0)
    grad_wx, grad_wh, grad_bias = gru_backward(grad_fresh, message, hidden_wide, stale_rows, gate_state)
    return (new_memory, embeddings, grad_wx, grad_wh, grad_bias) + weight_grads
```

```python
import functools
import math

import jax
import jax.numpy as jnp
from jax import lax
from jax.experimental import pallas as pl
from jax.experimental.pallas import tpu as pltpu
from jax.sharding import PartitionSpec as P


HEADS = 2
EPSILON = 1e-06
BUCKET = 160
ROWCAP = 384
SPILL = 200.0

BF = jnp.bfloat16
F32 = jnp.float32
I32 = jnp.int32


def matmul(left_side, right_side):
    return jnp.dot(left_side, right_side, preferred_element_type=F32)


def matmul_left(left_side, right_side):
    return lax.dot_general(
        left_side, right_side, (((0,), (0,)), ((), ())), preferred_element_type=F32
    )


def matmul_right(left_side, right_side):
    return lax.dot_general(
        left_side, right_side, (((1,), (1,)), ((), ())), preferred_element_type=F32
    )


def time_code(time_delta, time_freq):
    return jnp.cos(time_delta.astype(F32)[..., None] * time_freq).astype(BF)


def one_hot(condition):
    return jnp.where(condition, 1.0, 0.0).astype(BF)


def sub_iota(rows, lanes):
    return lax.broadcasted_iota(I32, (rows, lanes), 0).astype(F32)


def call(body, out_shape, args, scratch=(), scalars=0, flops=10**8):
    spaces = [pltpu.SMEM] * scalars + [pltpu.VMEM] * (len(args) - scalars)
    return pl.pallas_call(
        body,
        out_shape=out_shape,
        in_specs=[pl.BlockSpec(memory_space=space) for space in spaces],
        out_specs=jax.tree.map(lambda _: pl.BlockSpec(memory_space=pltpu.VMEM), out_shape),
        scratch_shapes=list(scratch),
        cost_estimate=pl.CostEstimate(flops=flops, transcendentals=0, bytes_accessed=10**6),
        compiler_params=pltpu.CompilerParams(vmem_limit_bytes=56 << 20),
    )(*args)


def shape(*dims, dtype=F32):
    return jax.ShapeDtypeStruct(dims, dtype)


def send(value, step, peers):
    return lax.ppermute(value, "emb", [(e, (e + step) % peers) for e in range(peers)])


def pack_body(feat_ref, req_ref, slot_ref, row_ref, dt_ref, count_ref, out_ref, req_scr):
    owners, slots, _ = feat_ref.shape
    capacity = req_ref.shape[1]
    width = req_scr.shape[1]
    req_scr[:, 0:capacity] = req_ref[...]
    slot = slot_ref[...].astype(F32)
    bucket = jnp.floor((slot + 0.5) * (1.0 / capacity))
    inside = slot - bucket * capacity + 1.0
    lane = lax.broadcasted_iota(I32, (1, width), 1).astype(F32)

    def step(o, carry):
        mine = jnp.where(bucket == o.astype(F32), inside, 0.0)
        filled = jnp.max(jnp.max(mine, axis=0, keepdims=True), axis=1, keepdims=True)
        asked = req_scr[pl.ds(o, 1), :]
        used = lane < filled
        high = jnp.where(used, (asked >> 6).astype(F32), 64.0)
        low = jnp.where(used, (asked & 63).astype(F32), 0.0)
        row = row_ref[pl.ds(o, 1), :]
        delta = dt_ref[pl.ds(o, 1), :]
        line = jnp.concatenate([row >> 6, row & 63, delta >> 5, delta & 31], axis=1).astype(F32)
        count = jnp.broadcast_to(count_ref[pl.ds(o, 1), :].astype(F32), (1, 128))
        block = jnp.concatenate(
            [high[:, b * 128 : (b + 1) * 128] for b in range(5)]
            + [low[:, b * 128 : (b + 1) * 128] for b in range(5)]
            + [line, count, jnp.zeros((4, 128), F32)],
            axis=0,
        )
        out_ref[o, 0:slots, :] = feat_ref[o]
        out_ref[o, slots:, :] = block.astype(BF)
        return carry

    lax.fori_loop(0, owners, step, 0, unroll=4)


def stale_body(target_ref, memory_ref, out_ref, half_ref):
    def take(i, carry):
        first = pl.multiple_of(i * 32, 32)
        rows = [memory_ref[pl.ds(target_ref[first + u], 1), :] for u in range(32)]
        rows = jnp.concatenate(rows, axis=0)
        out_ref[pl.ds(first, 32), :] = rows
        half_ref[pl.ds(first, 32), :] = rows.astype(BF)
        return carry

    lax.fori_loop(0, out_ref.shape[0] // 32, take, 0)


def route_body(feat_rows, msg_ref, code_ref, event_ref, rel_ref, rank_ref):
    sources = msg_ref.shape[0]
    slots = feat_rows
    width = rel_ref.shape[1]
    blocks = width // 128

    def table_step(s, table):
        block = msg_ref[s].astype(F32)
        high = block[slots + 10 : slots + 11, 0:slots]
        low = block[slots + 10 : slots + 11, slots : 2 * slots]
        count = block[slots + 11 : slots + 12, 0:slots]
        lane = lax.broadcasted_iota(I32, (1, slots), 1).astype(F32)
        live = lane < count
        high_hot = one_hot(sub_iota(64, slots) == high)
        low_hit = (sub_iota(64, slots) == low) & live
        first = jnp.where(low_hit, s.astype(F32) + 1.0, 0.0).astype(BF)
        second = jnp.where(low_hit, lane, 0.0).astype(BF)
        return table + matmul_right(jnp.concatenate([first, second], axis=0), high_hot)

    table = lax.fori_loop(
        0, sources, table_step, jnp.zeros((128, 64), F32), unroll=8
    ).astype(BF)

    def flat(s, first_row):
        block = msg_ref[s].astype(F32)
        return jnp.concatenate(
            [block[first_row + b : first_row + b + 1, :] for b in range(blocks)], axis=1
        )

    def find_step(s, carry):
        high = flat(s, slots)
        low = flat(s, slots + 5)
        high_hot = one_hot(sub_iota(64, width) == high)
        low_hit = sub_iota(64, width) == low
        found = matmul(table, high_hot)
        event_ref[pl.ds(s, 1), :] = jnp.sum(
            jnp.where(low_hit, found[0:64], 0.0), axis=0, keepdims=True
        )
        rank_ref[pl.ds(s, 1), :] = jnp.sum(
            jnp.where(low_hit, found[64:128], 0.0), axis=0, keepdims=True
        )
        return carry

    lax.fori_loop(0, sources, find_step, 0, unroll=4)
    first = event_ref[...]
    relevant = first > 0.0
    before = one_hot(
        lax.broadcasted_iota(I32, (width, width), 0) < lax.broadcasted_iota(I32, (width, width), 1)
    )
    rank = matmul(one_hot(relevant), before)
    event = (first - 1.0) * slots + rank_ref[...]
    code_ref[...] = jnp.where(
        relevant, jnp.where(rank < BUCKET, rank + 1.0, SPILL), 0.0
    ).astype(BF)
    event_ref[...] = jnp.where(relevant, event, -1.0)
    rel_ref[...] = jnp.where(relevant, rank, -1.0)


def compact_body(event_ref, rel_ref, index_ref):
    sources, width = rel_ref.shape

    def step(s, carry):
        rank = rel_ref[pl.ds(s, 1), :]
        event = event_ref[pl.ds(s, 1), :]
        hot = one_hot(sub_iota(BUCKET, width) == rank)
        high = jnp.floor(event * (1.0 / 32.0))
        low = event - high * 32.0
        have = jnp.where(rank >= 0.0, 1.0, 0.0)
        row = lax.broadcasted_iota(I32, (8, width), 0)
        digits = jnp.where(
            row == 0, high * have, jnp.where(row == 1, low * have, jnp.where(row == 2, have, 0.0))
        ).astype(BF)
        got = matmul_right(digits, hot)
        value = got[0:1] * 32.0 + got[1:2]
        index_ref[pl.ds(s, 1), :] = jnp.where(got[2:3] > 0.5, value, -1.0)
        return carry

    lax.fori_loop(0, sources, step, 0, unroll=4)


def picks_body(capacity, code_ref, slot_ref, rank_ref, sid_ref, flag_ref, got_ref):
    owners = code_ref.shape[0]
    peers, rows, lanes = slot_ref.shape
    table = jnp.concatenate([code_ref[:, b, :] for b in range(5)], axis=1).astype(BF)
    width = table.shape[1]

    def lookup(step, carry):
        peer = step // rows
        row = step % rows
        slot = slot_ref[peer, pl.ds(row, 1), :].astype(F32)
        owner = jnp.floor((slot + 0.5) * (1.0 / capacity))
        inside = slot - owner * capacity
        inside_hot = one_hot(sub_iota(width, lanes) == inside)
        found = matmul(table, inside_hot)
        mine = sub_iota(owners, lanes) == owner
        got = jnp.sum(jnp.where(mine, found, 0.0), axis=0, keepdims=True)
        got_ref[peer, pl.ds(row, 1), :] = jnp.where(slot >= 0.0, got, 0.0)
        return carry

    lax.fori_loop(0, peers * rows, lookup, 0, unroll=5)
    lane_before = one_hot(
        lax.broadcasted_iota(I32, (lanes, lanes), 0) < lax.broadcasted_iota(I32, (lanes, lanes), 1)
    )
    row_before = one_hot(
        lax.broadcasted_iota(I32, (rows, rows), 1) < lax.broadcasted_iota(I32, (rows, rows), 0)
    )
    ones = jnp.ones((lanes, lanes), BF)
    flag = jnp.zeros((8, lanes), F32)
    for peer in range(peers):
        got = got_ref[peer]
        relevant = got > 0.0
        hot = one_hot(relevant)
        rank = matmul(hot, lane_before) + matmul(row_before, matmul(hot, ones).astype(BF))
        rank = jnp.where(relevant, rank, -1.0)
        rank_ref[peer] = rank
        bad = jnp.where((got >= SPILL) | (rank >= ROWCAP), 1.0, 0.0)
        flag = jnp.maximum(flag, jnp.max(bad, axis=(0, 1), keepdims=True))
    flag_ref[...] = flag
    for peer in range(peers):

        def gather(row, total):
            slot = slot_ref[peer, pl.ds(row, 1), :].astype(F32)
            owner = jnp.floor((slot + 0.5) * (1.0 / capacity))
            rank = rank_ref[peer, pl.ds(row, 1), :]
            code = got_ref[peer, pl.ds(row, 1), :]
            have = jnp.where(rank >= 0.0, 1.0, 0.0)
            hot = one_hot(sub_iota(ROWCAP, lanes) == rank)
            line = lax.broadcasted_iota(I32, (8, lanes), 0)
            digits = jnp.where(
                line == 0,
                owner * have,
                jnp.where(line == 1, (code - 1.0) * have, jnp.where(line == 2, have, 0.0)),
            ).astype(BF)
            return total + matmul_right(digits, hot)

        total = lax.fori_loop(0, rows, gather, jnp.zeros((8, ROWCAP), F32), unroll=5)
        sid_ref[peer : peer + 1, :] = jnp.where(
            total[2:3] > 0.5, total[0:1] * BUCKET + total[1:2], -1.0
        )


def attend_body(
    keys,
    place_ref,
    part0_ref,
    part1_ref,
    part2_ref,
    part3_ref,
    code_ref,
    mask_ref,
    cot_ref,
    rank_ref,
    wq_ref,
    wk_ref,
    wv_ref,
    wt_ref,
    wo_ref,
    emb_ref,
    mix_ref,
    kg_ref,
    vg_ref,
    qg_ref,
    wide_ref,
    out0_ref,
    out1_ref,
    out2_ref,
    out3_ref,
    k_ref,
    v_ref,
    q_ref,
    g_ref,
    rq_ref,
    e_ref,
    r_ref,
    a_ref,
    d_ref,
    den_ref,
    dp_ref,
    mixf_ref,
    dq_ref,
    in_ref,
    back_ref,
):
    place = place_ref[0]
    nodes = cot_ref.shape[0]
    width = cot_ref.shape[1]
    half = width // HEADS
    chunk = 11 * nodes
    padded = kg_ref.shape[0]

    for step, part_ref in enumerate((part0_ref, part1_ref, part2_ref, part3_ref)):
        in_ref[(place + 4 - step) % 4] = part_ref[0 : keys * nodes, :]
    for e in range(4):
        wide_ref[:, e * 128 : (e + 1) * 128] = in_ref[e]

    def row_block(first, count):
        return wide_ref[pl.ds(first, count), :]

    def project(c, carry):
        at = pl.multiple_of(c * chunk, chunk)
        block = row_block(at, chunk)
        k_ref[pl.ds(at, chunk), :] = (
            matmul(block, wk_ref[...]) + matmul(code_ref[pl.ds(at, chunk), :], wt_ref[...])
        ).astype(BF)
        v_ref[pl.ds(at, chunk), :] = matmul(block, wv_ref[...]).astype(BF)
        return carry

    lax.fori_loop(0, keys // 11, project, 0)
    self_rows = row_block(0, nodes)
    query = matmul(self_rows, wq_ref[...]).astype(BF).astype(F32)
    g_ref[...] = matmul_right(cot_ref[...], wo_ref[...])
    for h in range(HEADS):
        part = query[:, h * half : (h + 1) * half]
        scale = lax.rsqrt(jnp.sum(part * part, axis=1, keepdims=True) * (1.0 / half) + EPSILON)
        rq_ref[:, h * 128 : (h + 1) * 128] = jnp.broadcast_to(scale, (nodes, 128))
        q_ref[:, h * half : (h + 1) * half] = part * scale

    tile = 16
    inv_root = 1.0 / math.sqrt(half)

    def wide(x):
        return jnp.concatenate([x, x], axis=1)

    for t in range(nodes // tile):
        lo = t * tile

        def forward(j, carry):
            at = pl.multiple_of(j * nodes + lo, tile)
            key = k_ref[pl.ds(at, tile), :].astype(F32)
            value = v_ref[pl.ds(at, tile), :].astype(F32)
            valid = mask_ref[pl.ds(at, tile), :]
            new = []
            for h in range(HEADS):
                den, dp, mixed = carry[h]
                cols = slice(h * half, (h + 1) * half)
                kh, vh = key[:, cols], value[:, cols]
                qh = q_ref[lo : lo + tile, cols]
                gh = g_ref[lo : lo + tile, cols]
                square = jnp.sum(kh * kh, axis=1, keepdims=True)
                inner = jnp.sum(qh * kh, axis=1, keepdims=True)
                toward = jnp.sum(gh * vh, axis=1, keepdims=True)
                square = jnp.broadcast_to(square, (tile, 128))
                inner = jnp.broadcast_to(inner, (tile, 128))
                toward = jnp.broadcast_to(toward, (tile, 128))
                scale = lax.rsqrt(square * (1.0 / half) + EPSILON)
                weight = jnp.exp(scale * inner * inv_root) * valid
                lanes = slice(h * 128, (h + 1) * 128)
                e_ref[pl.ds(at, tile), lanes] = weight
                r_ref[pl.ds(at, tile), lanes] = scale
                a_ref[pl.ds(at, tile), lanes] = inner
                d_ref[pl.ds(at, tile), lanes] = toward
                new.append((den + weight, dp + weight * toward, mixed + wide(weight) * vh))
            return tuple(new)

        zero = jnp.zeros((tile, 128), F32)
        start = tuple((zero, zero, jnp.zeros((tile, half), F32)) for _ in range(HEADS))
        done = lax.fori_loop(0, keys, forward, start, unroll=3)
        for h in range(HEADS):
            den, dp, mixed = done[h]
            inverse = 1.0 / den
            lanes = slice(h * 128, (h + 1) * 128)
            den_ref[lo : lo + tile, lanes] = inverse
            dp_ref[lo : lo + tile, lanes] = dp * inverse
            mixf_ref[lo : lo + tile, h * half : (h + 1) * half] = mixed * wide(inverse)

        def backward(j, carry):
            at = pl.multiple_of(j * nodes + lo, tile)
            key = k_ref[pl.ds(at, tile), :].astype(F32)
            new = []
            for h in range(HEADS):
                cols = slice(h * half, (h + 1) * half)
                lanes = slice(h * 128, (h + 1) * 128)
                kh = key[:, cols]
                qh = q_ref[lo : lo + tile, cols]
                gh = g_ref[lo : lo + tile, cols]
                weight = e_ref[pl.ds(at, tile), lanes] * den_ref[lo : lo + tile, lanes]
                scale = r_ref[pl.ds(at, tile), lanes]
                inner = a_ref[pl.ds(at, tile), lanes]
                toward = d_ref[pl.ds(at, tile), lanes]
                slope = weight * (toward - dp_ref[lo : lo + tile, lanes]) * inv_root
                along = slope * scale
                against = along * scale * scale * inner * (1.0 / half)
                along = wide(along)
                kg_ref[pl.ds(at, tile), cols] = (along * qh - wide(against) * kh).astype(BF)
                vg_ref[pl.ds(at, tile), cols] = (wide(weight) * gh).astype(BF)
                new.append(carry[h] + along * kh)
            return tuple(new)

        start = tuple(jnp.zeros((tile, half), F32) for _ in range(HEADS))
        done = lax.fori_loop(0, keys, backward, start, unroll=3)
        for h in range(HEADS):
            dq_ref[lo : lo + tile, h * half : (h + 1) * half] = done[h]

    tail = padded - keys * nodes
    kg_ref[keys * nodes :, :] = jnp.zeros((tail, width), BF)
    vg_ref[keys * nodes :, :] = jnp.zeros((tail, width), BF)
    for h in range(HEADS):
        cols = slice(h * half, (h + 1) * half)
        scale = wide(rq_ref[:, h * 128 : (h + 1) * 128])
        unit = q_ref[:, cols]
        slope = dq_ref[:, cols]
        inner = jnp.sum(slope * unit, axis=1, keepdims=True) * (1.0 / half)
        qg_ref[:, cols] = (scale * (slope - unit * inner)).astype(BF)
    mixed = mixf_ref[...].astype(BF)
    mix_ref[...] = mixed
    emb_ref[...] = (matmul(mixed, wo_ref[...]) + self_rows.astype(F32)).astype(BF)

    def pick(b, carry):
        keyed, valued = carry
        at = pl.multiple_of(b * 256, 256)
        rank = jnp.concatenate(
            [rank_ref[pl.ds(2 * b, 1), :], rank_ref[pl.ds(2 * b + 1, 1), :]], axis=1
        )
        hot = one_hot(sub_iota(ROWCAP, 256) == rank)
        keyed = keyed + matmul(hot, kg_ref[pl.ds(at, 256), :])
        valued = valued + matmul(hot, vg_ref[pl.ds(at, 256), :])
        return keyed, valued

    empty = jnp.zeros((ROWCAP, width), F32)
    keyed, valued = lax.fori_loop(0, padded // 256, pick, (empty, empty), unroll=3)
    hot = one_hot(sub_iota(ROWCAP, nodes) == rank_ref[0:1, 0:nodes])
    queried = matmul(hot, qg_ref[...]).astype(BF)
    total = (
        matmul_right(keyed.astype(BF), wk_ref[...])
        + matmul_right(valued.astype(BF), wv_ref[...])
        + (matmul_right(queried, wq_ref[...]) + matmul(hot, cot_ref[...]))
    ).astype(BF)
    for e in range(4):
        back_ref[e] = total[:, e * 128 : (e + 1) * 128]
    for step, out_ref in enumerate((out0_ref, out1_ref, out2_ref, out3_ref)):
        out_ref[...] = back_ref[(place + step) % 4]


def slots_body(place_ref, sid_ref, row0_ref, row1_ref, row2_ref, row3_ref, flag_ref, out_ref):
    place = place_ref[0]
    buckets = out_ref.shape[0]
    parts = (row0_ref, row1_ref, row2_ref, row3_ref)
    ids = jnp.concatenate(
        [sid_ref[pl.ds((place + 4 - step) % 4, 1), :] for step in range(4)], axis=1
    )
    data = jnp.concatenate([part[...] for part in parts], axis=0)
    flag = jnp.broadcast_to(flag_ref[0:1, :], (16, 128)).astype(BF)

    def step(o, carry):
        hot = one_hot(sub_iota(BUCKET, ids.shape[1]) + (o * BUCKET).astype(F32) == ids)
        out_ref[o, 0:BUCKET, :] = matmul(hot, data).astype(BF)
        out_ref[o, BUCKET:, :] = flag
        return carry

    lax.fori_loop(0, buckets, step, 0, unroll=4)


def events_body(index_ref, slots_ref, out_ref):
    events = out_ref.shape[0]
    turns, length = index_ref.shape
    each = length // BUCKET
    for half in range(2):
        base = half * (events // 2)

        def step(t, total):
            places = index_ref[pl.ds(t, 1), :] - base
            hot = one_hot(sub_iota(events // 2, length) == places)
            data = jnp.concatenate(
                [slots_ref[t * each + m, 0:BUCKET, :] for m in range(each)], axis=0
            )
            return total + matmul(hot, data)

        total = lax.fori_loop(0, turns, step, jnp.zeros((events // 2, 128), F32))
        out_ref[base : base + events // 2, :] = total


def refresh_body(
    target_ref, asked_ref, memory_ref, fresh_ref, code_ref, new_ref, out_ref
):
    new_ref[...] = memory_ref[...]
    events = fresh_ref.shape[0]
    owners, table_rows, _ = out_ref.shape
    capacity = table_rows - 16

    def put(i, carry):
        base = pl.multiple_of(i * 16, 16)
        for u in range(16):
            new_ref[pl.ds(target_ref[base + u], 1), :] = fresh_ref[pl.ds(base + u, 1), :]
        return carry

    lax.fori_loop(0, events // 16, put, 0)

    def take_owner(owner, carry):
        base = owner * table_rows

        def take(i, inner):
            first = pl.multiple_of(i * 32, 32)
            rows = [new_ref[pl.ds(asked_ref[base + first + u], 1), :] for u in range(32)]
            out_ref[owner, pl.ds(first, 32), :] = jnp.concatenate(rows, axis=0).astype(BF)
            return inner

        return lax.fori_loop(0, table_rows // 32, take, carry)

    lax.fori_loop(0, owners, take_owner, 0)
    for b in range(5):
        out_ref[:, capacity + b : capacity + b + 1, :] = code_ref[:, b : b + 1, :]
    out_ref[:, capacity + 5 :, :] = jnp.zeros((owners, 11, 128), BF)


def take_body(steps, place_ref, index_ref, table_ref, *refs):
    outs, full_ref = refs[:-1], refs[-1]
    full_ref[...] = table_ref[...].astype(F32)
    for step, out_ref in zip(steps, outs):
        count = out_ref.shape[0]
        start = ((place_ref[0] + step) % 4) * count

        def take(i, carry):
            first = pl.multiple_of(i * 32, 32)
            rows = [
                full_ref[pl.ds(index_ref[start + first + u], 1), :] for u in range(32)
            ]
            out_ref[pl.ds(first, 32), :] = jnp.concatenate(rows, axis=0).astype(BF)
            return carry

        lax.fori_loop(0, count // 32, take, 0)


def cell_body(
    place_ref,
    arrived_ref,
    code_ref,
    stale_ref,
    part0_ref,
    part1_ref,
    part2_ref,
    part3_ref,
    wx_ref,
    wh_ref,
    bias_ref,
    fresh_ref,
    reset_ref,
    update_ref,
    recall_ref,
    cand_ref,
    input_ref,
    wide_ref,
    in_ref,
):
    place = place_ref[0]
    sources = arrived_ref.shape[0]
    slots = stale_ref.shape[0] // sources
    for step, part_ref in enumerate((part0_ref, part1_ref, part2_ref, part3_ref)):
        in_ref[(place + 4 - step) % 4] = part_ref[...]
    for e in range(4):
        wide_ref[:, e * 128 : (e + 1) * 128] = in_ref[e]
    for s in range(sources):
        input_ref[s * slots : (s + 1) * slots, 0:128] = arrived_ref[s, 0:slots, :]
    input_ref[:, 128:256] = code_ref[...]
    chunk = 256

    def step(c, carry):
        at = pl.multiple_of(c * chunk, chunk)
        inputs = input_ref[pl.ds(at, chunk), :]
        hidden = wide_ref[pl.ds(at, chunk), :]
        stale = stale_ref[pl.ds(at, chunk), :]
        reset = jax.nn.sigmoid(
            matmul(inputs, wx_ref[0]) + matmul(hidden, wh_ref[0]) + bias_ref[0:1, :]
        )
        update = jax.nn.sigmoid(
            matmul(inputs, wx_ref[1]) + matmul(hidden, wh_ref[1]) + bias_ref[1:2, :]
        )
        recall = matmul(hidden, wh_ref[2]) + bias_ref[3:4, :]
        cand = jnp.tanh(matmul(inputs, wx_ref[2]) + bias_ref[2:3, :] + reset * recall)
        fresh = (1.0 - update) * cand + update * stale
        line = lax.broadcasted_iota(I32, (slots, 128), 0).astype(F32)
        live = jnp.concatenate(
            [
                jnp.where(
                    line
                    < arrived_ref[c * (chunk // slots) + k, slots + 8 : slots + 16, :].astype(F32)[
                        3:4
                    ],
                    1.0,
                    0.0,
                )
                for k in range(chunk // slots)
            ],
            axis=0,
        )
        fresh_ref[pl.ds(at, chunk), :] = jnp.where(live > 0.5, fresh, stale)
        reset_ref[pl.ds(at, chunk), :] = reset
        update_ref[pl.ds(at, chunk), :] = update
        recall_ref[pl.ds(at, chunk), :] = recall
        cand_ref[pl.ds(at, chunk), :] = cand
        return carry

    lax.fori_loop(0, stale_ref.shape[0] // chunk, step, 0)


def gates_body(
    grad_ref,
    input_ref,
    wide_ref,
    stale_ref,
    reset_ref,
    update_ref,
    recall_ref,
    cand_ref,
    out_ref,
):
    grad = grad_ref[...]
    reset, update = reset_ref[...], update_ref[...]
    recall, cand = recall_ref[...], cand_ref[...]
    cand_term = grad * (1.0 - update) * (1.0 - cand * cand)
    update_term = grad * (stale_ref[...] - cand) * update * (1.0 - update)
    recall_term = cand_term * reset
    reset_term = cand_term * recall * reset * (1.0 - reset)
    terms = [reset_term, update_term, cand_term, recall_term]
    rounded = [term.astype(BF) for term in terms]
    seen = input_ref.shape[1]
    known = wide_ref.shape[1]
    left = jnp.concatenate(rounded[0:3], axis=1)
    right = jnp.concatenate([rounded[0], rounded[1], rounded[3]], axis=1)
    from_input = matmul_left(input_ref[...], left).astype(BF)
    from_wide = matmul_left(wide_ref[...], right).astype(BF)
    for g in range(3):
        lanes = slice(g * 128, (g + 1) * 128)
        out_ref[g * seen : (g + 1) * seen, :] = from_input[:, lanes]
        out_ref[3 * seen + g * known : 3 * seen + (g + 1) * known, :] = from_wide[:, lanes]
    first = 3 * (seen + known)
    sums = jnp.concatenate(
        [jnp.sum(term, axis=0, keepdims=True) for term in terms] + [jnp.zeros((12, 128), F32)],
        axis=0,
    )
    out_ref[first : first + 16, :] = sums.astype(BF)
    out_ref[first + 16 :, :] = jnp.zeros((out_ref.shape[0] - first - 16, 128), BF)


def weights_body(
    count,
    place_ref,
    wide_ref,
    code_ref,
    mix_ref,
    cot_ref,
    kg_ref,
    vg_ref,
    qg_ref,
    out0_ref,
    out1_ref,
    out2_ref,
    out3_ref,
    block_ref,
):
    place = place_ref[0]
    width = cot_ref.shape[1]
    nodes = cot_ref.shape[0]

    def keep(first, value):
        for e in range(4):
            block_ref[e, first : first + value.shape[0], :] = value[
                :, e * 128 : (e + 1) * 128
            ].astype(BF)

    rows = wide_ref[...]
    keep(0, matmul_left(rows[0:nodes, :], qg_ref[...]))
    keep(width, matmul_left(rows, kg_ref[0:count, :]))
    keep(2 * width, matmul_left(rows, vg_ref[0:count, :]))
    keep(3 * width, matmul_left(code_ref[...], kg_ref[0:count, :]))
    keep(3 * width + 128, matmul_left(mix_ref[...], cot_ref[...]))
    for step, out_ref in enumerate((out0_ref, out1_ref, out2_ref, out3_ref)):
        out_ref[...] = block_ref[(place + step) % 4]


def spread_body(place_ref, b0, b1, b2, b3, query_ref, key_ref, value_ref, time_ref, out_ref, block):
    place = place_ref[0]
    for step, part_ref in enumerate((b0, b1, b2, b3)):
        block[(place + 4 - step) % 4] = part_ref[0 : block.shape[1], :]
    first = 0
    for ref in (query_ref, key_ref, value_ref, time_ref, out_ref):
        for e in range(4):
            ref[:, e * 128 : (e + 1) * 128] = block[e, first : first + ref.shape[0], :].astype(F32)
        first += ref.shape[0]


def exchange(value, axes):
    return lax.all_to_all(value, axes, split_axis=0, concat_axis=0, tiled=True)


def reduce_mem(value, count):
    parts = value.reshape(count, value.shape[0] // count, value.shape[1])
    arrived = exchange(parts, "mem")
    summed = jnp.sum(arrived.astype(F32), axis=0).astype(BF)
    gathered = exchange(jnp.broadcast_to(summed[None], parts.shape), "mem")
    return gathered.reshape(value.shape)


def per_device(
    memory,
    ev_rows,
    ev_count,
    ev_feat,
    ev_dt,
    req_rows,
    nbr_slot,
    nbr_dt,
    nbr_len,
    time_freq,
    gru_wx,
    gru_wh,
    gru_bias,
    w_query,
    w_key,
    w_value,
    w_time,
    w_out,
    cotangent,
):
    columns = memory.shape[1]
    rows_dev = memory.shape[0]
    owners, slot_count = ev_rows.shape[1], ev_rows.shape[2]
    capacity = req_rows.shape[2]
    batch, keys = nbr_slot.shape
    nodes = nbr_len.shape[0]
    peers = batch // nodes
    width = columns * peers
    flat_slots = 640
    table_rows = capacity + 16
    picks = 2176

    packed = call(
        pack_body,
        shape(owners, slot_count + 16, 128, dtype=BF),
        (ev_feat[0], req_rows[0], nbr_slot, ev_rows[0], ev_dt[0], ev_count.reshape(owners, 1)),
        [pltpu.VMEM((owners, flat_slots), I32)],
    )
    arrived = exchange(packed, "mem")

    line = arrived[:, slot_count + 10, :].astype(I32)
    targets = (line[:, :slot_count] * 64 + line[:, slot_count : 2 * slot_count]).reshape(-1)
    deltas = line[:, 2 * slot_count : 3 * slot_count] * 32 + line[:, 3 * slot_count :]
    live_counts = arrived[:, slot_count + 11, 0:1].astype(I32)
    live_mask = (jnp.arange(slot_count, dtype=I32)[None, :] < live_counts).reshape(-1)
    asked = (
        arrived[:, slot_count : slot_count + 5, :].astype(I32) * 64
        + arrived[:, slot_count + 5 : slot_count + 10, :].astype(I32)
    ).reshape(owners, flat_slots)
    asked = jnp.minimum(asked[:, :table_rows], rows_dev - 1)

    place = lax.axis_index("emb").astype(I32).reshape(1)
    total_events = owners * slot_count
    stale_rows, stale_half = call(
        stale_body,
        (shape(total_events, columns), shape(total_events, columns, dtype=BF)),
        (targets, memory),
        scalars=1,
    )
    wide_parts = [stale_half] + [send(stale_half, step, peers) for step in (1, 2, 3)]
    codes_event = time_code(deltas.reshape(-1), time_freq)
    codes, events, ranks = call(
        functools.partial(route_body, slot_count),
        (
            jax.ShapeDtypeStruct((owners, flat_slots), BF),
            jax.ShapeDtypeStruct((owners, flat_slots), F32),
            jax.ShapeDtypeStruct((owners, flat_slots), F32),
        ),
        (arrived,),
        [pltpu.VMEM((owners, flat_slots), F32)],
    )
    index = call(compact_body, jax.ShapeDtypeStruct((owners, BUCKET), F32), (events, ranks))
    fresh_rows, reset, update, recall, cand, inputs, hidden_wide = call(
        cell_body,
        (shape(total_events, columns),) * 5
        + (shape(total_events, 256, dtype=BF), shape(total_events, width, dtype=BF)),
        (place, arrived, codes_event, stale_rows, *wide_parts, gru_wx, gru_wh, gru_bias),
        [pltpu.VMEM((peers, total_events, columns), BF)],
        scalars=1,
    )
    new_memory, outgoing = call(
        refresh_body,
        (shape(rows_dev, columns), shape(owners, table_rows, columns, dtype=BF)),
        (
            targets,
            asked.reshape(-1),
            memory,
            fresh_rows,
            codes.reshape(owners, 5, 128),
        ),
        scalars=2,
    )
    fetched = exchange(outgoing, "mem")

    ordered = jnp.transpose(nbr_slot.reshape(peers, nodes, keys), (0, 2, 1)).reshape(peers, -1)
    count = keys * nodes
    row_index = jnp.pad(ordered + 16 * (ordered // capacity), ((0, 0), (0, picks - count)))
    table = fetched.reshape(-1, columns)
    part = shape(picks, columns, dtype=BF)
    row_index = row_index.reshape(-1)

    def taken(steps):
        return call(
            functools.partial(take_body, steps),
            (part,) * len(steps),
            (place, row_index, table),
            [pltpu.VMEM(table.shape, F32)],
            scalars=2,
        )

    near, far = taken((1, 2))
    near = send(near, 1, peers)
    far = send(far, 2, peers)
    last, own = taken((3, 0))
    last = send(last, 3, peers)

    slots_in = jnp.pad(ordered, ((0, 0), (0, 24 * 128 - count)), constant_values=-1)
    slots_in = slots_in.reshape(peers, 24, 128)
    pick_rank, slot_list, flag = call(
        functools.partial(picks_body, capacity),
        (
            jax.ShapeDtypeStruct((peers, 24, 128), F32),
            jax.ShapeDtypeStruct((peers, ROWCAP), F32),
            jax.ShapeDtypeStruct((8, 128), F32),
        ),
        (fetched[:, capacity:, :].astype(F32), slots_in),
        [pltpu.VMEM((peers, 24, 128), F32)],
    )
    my_rank = lax.dynamic_index_in_dim(pick_rank, lax.axis_index("emb"), 0, keepdims=False)

    position = jnp.arange(keys, dtype=I32)[:, None]
    valid = (position <= nbr_len[None, :]).astype(F32).reshape(-1, 1)
    valid = jnp.broadcast_to(valid, (count, 128))
    codes_in = time_code(jnp.transpose(nbr_dt).reshape(-1), time_freq)
    padded = 2304
    embedding, mixed, key_grad, value_grad, query_grad, rows_wide, *compact_rows = call(
        functools.partial(attend_body, keys),
        (
            jax.ShapeDtypeStruct((nodes, width), BF),
            jax.ShapeDtypeStruct((nodes, width), BF),
            jax.ShapeDtypeStruct((padded, width), BF),
            jax.ShapeDtypeStruct((padded, width), BF),
            jax.ShapeDtypeStruct((nodes, width), BF),
            jax.ShapeDtypeStruct((count, width), BF),
        )
        + (shape(ROWCAP, columns, dtype=BF),) * 4,
        (
            place,
            own,
            near,
            far,
            last,
            codes_in,
            valid,
            cotangent,
            my_rank,
            w_query,
            w_key,
            w_value,
            w_time,
            w_out,
        ),
        [
            pltpu.VMEM((count, width), BF),
            pltpu.VMEM((count, width), BF),
            pltpu.VMEM((nodes, width), F32),
            pltpu.VMEM((nodes, width), F32),
            pltpu.VMEM((nodes, 256), F32),
            pltpu.VMEM((count, 256), F32),
            pltpu.VMEM((count, 256), F32),
            pltpu.VMEM((count, 256), F32),
            pltpu.VMEM((count, 256), F32),
            pltpu.VMEM((nodes, 256), F32),
            pltpu.VMEM((nodes, 256), F32),
            pltpu.VMEM((nodes, width), F32),
            pltpu.VMEM((nodes, width), F32),
            pltpu.VMEM((peers, count, columns), BF),
            pltpu.VMEM((peers, ROWCAP, columns), BF),
        ],
        scalars=1,
        flops=8 * 10**9,
    )

    returned_rows = compact_rows[:1]
    for step in (1, 2, 3):
        returned_rows.append(send(compact_rows[step], step, peers))
    slot_sums = call(
        slots_body,
        shape(owners, BUCKET + 16, columns, dtype=BF),
        (place, slot_list, *returned_rows, flag),
        scalars=1,
    )
    returned = exchange(slot_sums, "mem")
    spilled = jnp.max(returned[:, BUCKET, 0].astype(F32)) > 0.0
    sparse_grad = call(events_body, shape(total_events, columns), (index.reshape(8, -1), returned))

    def dense_grad(_):
        key_rows, value_rows = key_grad[:count], value_grad[:count]
        grad = matmul_right(key_rows, w_key) + matmul_right(value_rows, w_value)
        own = matmul_right(query_grad, w_query) + cotangent.astype(F32)
        grad = grad.at[:nodes].add(own).astype(BF)
        parts = jnp.transpose(grad.reshape(count, peers, columns), (1, 0, 2))
        parts = exchange(parts, "emb").reshape(-1, columns).astype(F32)
        sums = jnp.zeros((owners * capacity, columns), F32).at[ordered.reshape(-1)].add(parts)
        back = exchange(sums.astype(BF).reshape(owners, capacity, columns), "mem")
        table = jnp.zeros_like(memory).at[asked[:, :capacity].reshape(-1)].add(
            back.reshape(-1, columns).astype(F32)
        )
        return jnp.where(live_mask[:, None], table[targets], 0.0)

    grad_fresh = lax.cond(spilled, dense_grad, lambda kept: kept, sparse_grad)

    total_weight = 3 * width + 128 + width
    shard = owners * 80
    weight_parts = call(
        functools.partial(weights_body, count),
        (shape(total_weight, columns, dtype=BF),) * 4,
        (
            place,
            rows_wide,
            codes_in,
            mixed,
            cotangent,
            key_grad,
            value_grad,
            query_grad,
        ),
        [pltpu.VMEM((peers, total_weight, columns), BF)],
        scalars=1,
        flops=2 * 10**9,
    )
    weight_sum = weight_parts[0].astype(F32)
    for step in (1, 2, 3):
        moved = send(weight_parts[step], step, peers)
        weight_sum = weight_sum + moved.astype(F32)
    weight_sum = jnp.pad(weight_sum.astype(BF), ((0, shard - total_weight), (0, 0)))
    weight_sum = reduce_mem(weight_sum, owners)[:total_weight]
    spread_parts = []
    for step in (1, 2, 3):
        spread_parts.append(send(weight_sum, step, peers))
    grad_query, grad_key, grad_value, grad_time, grad_out = call(
        spread_body,
        (
            shape(width, width),
            shape(width, width),
            shape(width, width),
            shape(128, width),
            shape(width, width),
        ),
        (place, weight_sum, *spread_parts),
        [pltpu.VMEM((peers, total_weight, columns), BF)],
        scalars=1,
    )

    gate_rows = call(
        gates_body,
        shape(shard, columns, dtype=BF),
        (grad_fresh, inputs, hidden_wide, stale_rows, reset, update, recall, cand),
    )
    gate_rows = reduce_mem(gate_rows, owners).astype(F32)
    split = 3 * 256
    grad_wx = gate_rows[:split].reshape(gru_wx.shape)
    grad_wh = gate_rows[split : split + 3 * width].reshape(gru_wh.shape)
    grad_bias = gate_rows[split + 3 * width : split + 3 * width + 4]
    return (
        new_memory,
        embedding,
        grad_wx,
        grad_wh,
        grad_bias,
        grad_query,
        grad_key,
        grad_value,
        grad_time,
        grad_out,
    )


def solution(mesh):
    in_specs = (
        P("mem", "emb"),
        P("mem", None, None),
        P("mem", None),
        P("mem", None, None, None),
        P("mem", None, None),
        P("mem", None, None),
        P("mem", None),
        P(("mem", "emb"), None),
        P(("mem", "emb")),
        P(),
        P(None, None, "emb"),
        P(None, None, "emb"),
        P(None, "emb"),
        P(),
        P(),
        P(),
        P(),
        P(),
        P(("mem", "emb"), None),
    )
    out_specs = (
        P("mem", "emb"),
        P(("mem", "emb"), None),
        P(None, None, "emb"),
        P(None, None, "emb"),
        P(None, "emb"),
        P(),
        P(),
        P(),
        P(),
        P(),
    )

    return jax.shard_map(
        per_device, mesh=mesh, in_specs=in_specs, out_specs=out_specs, check_vma=False
    )
```

```python
import functools
import math

import jax
import jax.numpy as jnp
from jax import lax
from jax.experimental import pallas as pl
from jax.experimental.pallas import tpu as pltpu
from jax.sharding import PartitionSpec as P


HEADS = 2
EPSILON = 1e-06
BUCKET = 160
ROWCAP = 384
SPILL = 200.0

BF = jnp.bfloat16
F32 = jnp.float32
I32 = jnp.int32


def matmul(left_side, right_side):
    return jnp.dot(left_side, right_side, preferred_element_type=F32)


def matmul_left(left_side, right_side):
    return lax.dot_general(
        left_side, right_side, (((0,), (0,)), ((), ())), preferred_element_type=F32
    )


def matmul_right(left_side, right_side):
    return lax.dot_general(
        left_side, right_side, (((1,), (1,)), ((), ())), preferred_element_type=F32
    )


def time_code(time_delta, time_freq):
    return jnp.cos(time_delta.astype(F32)[..., None] * time_freq).astype(BF)


def one_hot(condition):
    return jnp.where(condition, 1.0, 0.0).astype(BF)


def sub_iota(rows, lanes):
    return lax.broadcasted_iota(I32, (rows, lanes), 0).astype(F32)


def call(body, out_shape, args, scratch=(), scalars=0, flops=10**8):
    spaces = [pltpu.SMEM] * scalars + [pltpu.VMEM] * (len(args) - scalars)
    return pl.pallas_call(
        body,
        out_shape=out_shape,
        in_specs=[pl.BlockSpec(memory_space=space) for space in spaces],
        out_specs=jax.tree.map(lambda _: pl.BlockSpec(memory_space=pltpu.VMEM), out_shape),
        scratch_shapes=list(scratch),
        cost_estimate=pl.CostEstimate(flops=flops, transcendentals=0, bytes_accessed=10**6),
        compiler_params=pltpu.CompilerParams(vmem_limit_bytes=56 << 20),
    )(*args)


def shape(*dims, dtype=F32):
    return jax.ShapeDtypeStruct(dims, dtype)


def send(value, step, peers):
    return lax.ppermute(value, "emb", [(e, (e + step) % peers) for e in range(peers)])


def pack_body(feat_ref, req_ref, slot_ref, row_ref, dt_ref, count_ref, out_ref, req_scr):
    owners, slots, _ = feat_ref.shape
    capacity = req_ref.shape[1]
    width = req_scr.shape[1]
    req_scr[:, 0:capacity] = req_ref[...]
    slot = slot_ref[...].astype(F32)
    bucket = jnp.floor((slot + 0.5) * (1.0 / capacity))
    inside = slot - bucket * capacity + 1.0
    counts = count_ref[...].astype(F32)
    owner_lane = lax.broadcasted_iota(I32, counts.shape, 1)
    lane = lax.broadcasted_iota(I32, (1, width), 1).astype(F32)

    def step(o, carry):
        mine = jnp.where(bucket == o.astype(F32), inside, 0.0)
        filled = jnp.max(jnp.max(mine, axis=0, keepdims=True), axis=1, keepdims=True)
        asked = req_scr[pl.ds(o, 1), :]
        used = lane < filled
        high = jnp.where(used, (asked >> 6).astype(F32), 64.0)
        low = jnp.where(used, (asked & 63).astype(F32), 0.0)
        row = row_ref[pl.ds(o, 1), :]
        delta = dt_ref[pl.ds(o, 1), :]
        line = jnp.concatenate([row >> 6, row & 63, delta >> 5, delta & 31], axis=1).astype(F32)
        count = jnp.sum(jnp.where(owner_lane == o, counts, 0.0), axis=1, keepdims=True)
        count = jnp.broadcast_to(count, (1, 128))
        block = jnp.concatenate(
            [high[:, b * 128 : (b + 1) * 128] for b in range(5)]
            + [low[:, b * 128 : (b + 1) * 128] for b in range(5)]
            + [line, count, jnp.zeros((4, 128), F32)],
            axis=0,
        )
        out_ref[o, 0:slots, :] = feat_ref[o]
        out_ref[o, slots:, :] = block.astype(BF)
        return carry

    lax.fori_loop(0, owners, step, 0, unroll=4)


def stale_body(target_ref, memory_ref, out_ref, half_ref):
    def take(i, carry):
        first = pl.multiple_of(i * 32, 32)
        rows = [memory_ref[pl.ds(target_ref[first + u], 1), :] for u in range(32)]
        rows = jnp.concatenate(rows, axis=0)
        out_ref[pl.ds(first, 32), :] = rows
        half_ref[pl.ds(first, 32), :] = rows.astype(BF)
        return carry

    lax.fori_loop(0, out_ref.shape[0] // 32, take, 0)


def route_body(feat_rows, msg_ref, code_ref, event_ref, rel_ref, rank_ref):
    sources = msg_ref.shape[0]
    slots = feat_rows
    width = rel_ref.shape[1]
    blocks = width // 128

    def table_step(s, table):
        block = msg_ref[s].astype(F32)
        high = block[slots + 10 : slots + 11, 0:slots]
        low = block[slots + 10 : slots + 11, slots : 2 * slots]
        count = block[slots + 11 : slots + 12, 0:slots]
        lane = lax.broadcasted_iota(I32, (1, slots), 1).astype(F32)
        live = lane < count
        high_hot = one_hot(sub_iota(64, slots) == high)
        low_hit = (sub_iota(64, slots) == low) & live
        first = jnp.where(low_hit, s.astype(F32) + 1.0, 0.0).astype(BF)
        second = jnp.where(low_hit, lane, 0.0).astype(BF)
        return table + matmul_right(jnp.concatenate([first, second], axis=0), high_hot)

    table = lax.fori_loop(
        0, sources, table_step, jnp.zeros((128, 64), F32), unroll=8
    ).astype(BF)

    def flat(s, first_row):
        block = msg_ref[s].astype(F32)
        return jnp.concatenate(
            [block[first_row + b : first_row + b + 1, :] for b in range(blocks)], axis=1
        )

    def find_step(s, carry):
        high = flat(s, slots)
        low = flat(s, slots + 5)
        high_hot = one_hot(sub_iota(64, width) == high)
        low_hit = sub_iota(64, width) == low
        found = matmul(table, high_hot)
        event_ref[pl.ds(s, 1), :] = jnp.sum(
            jnp.where(low_hit, found[0:64], 0.0), axis=0, keepdims=True
        )
        rank_ref[pl.ds(s, 1), :] = jnp.sum(
            jnp.where(low_hit, found[64:128], 0.0), axis=0, keepdims=True
        )
        return carry

    lax.fori_loop(0, sources, find_step, 0, unroll=4)
    first = event_ref[...]
    relevant = first > 0.0
    before = one_hot(
        lax.broadcasted_iota(I32, (width, width), 0) < lax.broadcasted_iota(I32, (width, width), 1)
    )
    rank = matmul(one_hot(relevant), before)
    event = (first - 1.0) * slots + rank_ref[...]
    code_ref[...] = jnp.where(
        relevant, jnp.where(rank < BUCKET, rank + 1.0, SPILL), 0.0
    )
    event_ref[...] = jnp.where(relevant, event, -1.0)
    rel_ref[...] = jnp.where(relevant, rank, -1.0)


def compact_body(event_ref, rel_ref, index_ref):
    _, width = rel_ref.shape
    turns, length = index_ref.shape
    each = length // BUCKET

    def step(t, carry):
        lines = []
        for m in range(each):
            rank = rel_ref[pl.ds(t * each + m, 1), :]
            event = event_ref[pl.ds(t * each + m, 1), :]
            hot = one_hot(sub_iota(BUCKET, width) == rank)
            high = jnp.floor(event * (1.0 / 32.0))
            low = event - high * 32.0
            have = jnp.where(rank >= 0.0, 1.0, 0.0)
            row = lax.broadcasted_iota(I32, (8, width), 0)
            digits = jnp.where(
                row == 0,
                high * have,
                jnp.where(row == 1, low * have, jnp.where(row == 2, have, 0.0)),
            ).astype(BF)
            got = matmul_right(digits, hot)
            lines.append(jnp.where(got[2:3] > 0.5, got[0:1] * 32.0 + got[1:2], -1.0))
        index_ref[pl.ds(t, 1), :] = jnp.concatenate(lines, axis=1)
        return carry

    lax.fori_loop(0, turns, step, 0)


def picks_body(capacity, code_ref, slot_ref, rank_ref, sid_ref, flag_ref, got_ref):
    owners, width = code_ref.shape
    peers, rows, lanes = slot_ref.shape
    fine = 16
    coarse = width // fine
    codes = code_ref[...].astype(BF)
    spot = lax.broadcasted_iota(I32, (width, 128), 0)
    column = lax.broadcasted_iota(I32, (width, 128), 1)
    table = jnp.concatenate(
        [matmul(codes, one_hot(spot == column * fine + low)) for low in range(fine)], axis=0
    ).astype(BF)[:, 0:coarse]

    def pair(ref, peer, row):
        return jnp.concatenate(
            [ref[peer, pl.ds(row, 1), :], ref[peer, pl.ds(row + 1, 1), :]], axis=1
        )

    def place_of(slot):
        owner = jnp.floor((slot + 0.5) * (1.0 / capacity))
        return owner, slot - owner * capacity

    def lookup(step, carry):
        peer = step // 9
        row = (step % 9) * 2
        slot = pair(slot_ref, peer, row).astype(F32)
        owner, inside = place_of(slot)
        high = jnp.floor(inside * (1.0 / fine))
        found = matmul(table, one_hot(sub_iota(coarse, 2 * lanes) == high))
        mine = sub_iota(fine * owners, 2 * lanes) == (inside - high * fine) * owners + owner
        got = jnp.sum(jnp.where(mine, found, 0.0), axis=0, keepdims=True)
        got = jnp.where(slot >= 0.0, got, 0.0)
        got_ref[peer, pl.ds(row, 1), :] = got[:, 0:lanes]
        got_ref[peer, pl.ds(row + 1, 1), :] = got[:, lanes:]
        return carry

    got_ref[:, 16:24, :] = jnp.zeros((peers, 8, lanes), F32)
    lax.fori_loop(0, peers * 9, lookup, 0, unroll=4)
    lane_before = one_hot(
        lax.broadcasted_iota(I32, (lanes, lanes), 0) < lax.broadcasted_iota(I32, (lanes, lanes), 1)
    )
    row_before = one_hot(
        lax.broadcasted_iota(I32, (rows, rows), 1) < lax.broadcasted_iota(I32, (rows, rows), 0)
    )
    ones = jnp.ones((lanes, lanes), BF)
    flag = jnp.zeros((8, lanes), F32)
    for peer in range(peers):
        got = got_ref[peer]
        relevant = got > 0.0
        hot = one_hot(relevant)
        rank = matmul(hot, lane_before) + matmul(row_before, matmul(hot, ones).astype(BF))
        rank = jnp.where(relevant, rank, -1.0)
        rank_ref[peer] = rank
        bad = jnp.where((got >= SPILL) | (rank >= ROWCAP), 1.0, 0.0)
        flag = jnp.maximum(flag, jnp.max(bad, axis=(0, 1), keepdims=True))
    flag_ref[...] = flag
    for peer in range(peers):

        def gather(step, total):
            row = step * 2
            owner, _ = place_of(pair(slot_ref, peer, row).astype(F32))
            rank = pair(rank_ref, peer, row)
            code = pair(got_ref, peer, row)
            have = jnp.where(rank >= 0.0, 1.0, 0.0)
            hot = one_hot(sub_iota(ROWCAP, 2 * lanes) == rank)
            line = lax.broadcasted_iota(I32, (128, 2 * lanes), 0)
            digits = jnp.where(
                line == 0,
                owner * have,
                jnp.where(line == 1, (code - 1.0) * have, jnp.where(line == 2, have, 0.0)),
            ).astype(BF)
            return total + matmul_right(hot, digits)

        total = lax.fori_loop(0, 9, gather, jnp.zeros((ROWCAP, 128), F32), unroll=3)
        total = jnp.transpose(total)
        sid_ref[peer : peer + 1, :] = jnp.where(
            total[2:3] > 0.5, total[0:1] * BUCKET + total[1:2], -1.0
        )


def attend_body(
    keys,
    place_ref,
    part0_ref,
    part1_ref,
    part2_ref,
    part3_ref,
    code_ref,
    mask_ref,
    cot_ref,
    rank_ref,
    wq_ref,
    wk_ref,
    wv_ref,
    wt_ref,
    wo_ref,
    emb_ref,
    mix_ref,
    kg_ref,
    vg_ref,
    qg_ref,
    wide_ref,
    out0_ref,
    out1_ref,
    out2_ref,
    out3_ref,
    k_ref,
    v_ref,
    q_ref,
    g_ref,
    rq_ref,
    e_ref,
    r_ref,
    a_ref,
    d_ref,
    den_ref,
    dp_ref,
    mixf_ref,
    dq_ref,
    in_ref,
    back_ref,
):
    place = place_ref[0]
    nodes = cot_ref.shape[0]
    width = cot_ref.shape[1]
    half = width // HEADS
    chunk = 11 * nodes
    padded = kg_ref.shape[0]

    for step, part_ref in enumerate((part0_ref, part1_ref, part2_ref, part3_ref)):
        in_ref[(place + 4 - step) % 4] = part_ref[0 : keys * nodes, :]
    for e in range(4):
        wide_ref[:, e * 128 : (e + 1) * 128] = in_ref[e]

    def row_block(first, count):
        return wide_ref[pl.ds(first, count), :]

    def project(c, carry):
        at = pl.multiple_of(c * chunk, chunk)
        block = row_block(at, chunk)
        k_ref[pl.ds(at, chunk), :] = (
            matmul(block, wk_ref[...]) + matmul(code_ref[pl.ds(at, chunk), :], wt_ref[...])
        ).astype(BF)
        v_ref[pl.ds(at, chunk), :] = matmul(block, wv_ref[...]).astype(BF)
        return carry

    lax.fori_loop(0, keys // 11, project, 0)
    self_rows = row_block(0, nodes)
    query = matmul(self_rows, wq_ref[...]).astype(BF).astype(F32)
    g_ref[...] = matmul_right(cot_ref[...], wo_ref[...])
    for h in range(HEADS):
        part = query[:, h * half : (h + 1) * half]
        scale = lax.rsqrt(jnp.sum(part * part, axis=1, keepdims=True) * (1.0 / half) + EPSILON)
        rq_ref[:, h * 128 : (h + 1) * 128] = jnp.broadcast_to(scale, (nodes, 128))
        q_ref[:, h * half : (h + 1) * half] = part * scale

    tile = 16
    inv_root = 1.0 / math.sqrt(half)

    def wide(x):
        return jnp.concatenate([x, x], axis=1)

    def tile_step(t, outer):
        lo = pl.multiple_of(t * tile, tile)
        rows = pl.ds(lo, tile)

        def forward(j, carry):
            at = pl.multiple_of(j * nodes + lo, tile)
            key = k_ref[pl.ds(at, tile), :].astype(F32)
            value = v_ref[pl.ds(at, tile), :].astype(F32)
            valid = jnp.where(j.astype(F32) <= mask_ref[rows, :], 1.0, 0.0)
            new = []
            for h in range(HEADS):
                den, dp, mixed = carry[h]
                cols = slice(h * half, (h + 1) * half)
                kh, vh = key[:, cols], value[:, cols]
                qh = q_ref[rows, cols]
                gh = g_ref[rows, cols]
                square = jnp.sum(kh * kh, axis=1, keepdims=True)
                inner = jnp.sum(qh * kh, axis=1, keepdims=True)
                toward = jnp.sum(gh * vh, axis=1, keepdims=True)
                square = jnp.broadcast_to(square, (tile, 128))
                inner = jnp.broadcast_to(inner, (tile, 128))
                toward = jnp.broadcast_to(toward, (tile, 128))
                scale = lax.rsqrt(square * (1.0 / half) + EPSILON)
                weight = jnp.exp(scale * inner * inv_root) * valid
                lanes = slice(h * 128, (h + 1) * 128)
                e_ref[pl.ds(at, tile), lanes] = weight
                r_ref[pl.ds(at, tile), lanes] = scale
                a_ref[pl.ds(at, tile), lanes] = inner
                d_ref[pl.ds(at, tile), lanes] = toward
                new.append((den + weight, dp + weight * toward, mixed + wide(weight) * vh))
            return tuple(new)

        zero = jnp.zeros((tile, 128), F32)
        start = tuple((zero, zero, jnp.zeros((tile, half), F32)) for _ in range(HEADS))
        done = lax.fori_loop(0, keys, forward, start, unroll=3)
        for h in range(HEADS):
            den, dp, mixed = done[h]
            inverse = 1.0 / den
            lanes = slice(h * 128, (h + 1) * 128)
            den_ref[rows, lanes] = inverse
            dp_ref[rows, lanes] = dp * inverse
            mixf_ref[rows, h * half : (h + 1) * half] = mixed * wide(inverse)

        def backward(j, carry):
            at = pl.multiple_of(j * nodes + lo, tile)
            key = k_ref[pl.ds(at, tile), :].astype(F32)
            new = []
            for h in range(HEADS):
                cols = slice(h * half, (h + 1) * half)
                lanes = slice(h * 128, (h + 1) * 128)
                kh = key[:, cols]
                qh = q_ref[rows, cols]
                gh = g_ref[rows, cols]
                weight = e_ref[pl.ds(at, tile), lanes] * den_ref[rows, lanes]
                scale = r_ref[pl.ds(at, tile), lanes]
                inner = a_ref[pl.ds(at, tile), lanes]
                toward = d_ref[pl.ds(at, tile), lanes]
                slope = weight * (toward - dp_ref[rows, lanes]) * inv_root
                along = slope * scale
                against = along * scale * scale * inner * (1.0 / half)
                along = wide(along)
                kg_ref[pl.ds(at, tile), cols] = (along * qh - wide(against) * kh).astype(BF)
                vg_ref[pl.ds(at, tile), cols] = (wide(weight) * gh).astype(BF)
                new.append(carry[h] + along * kh)
            return tuple(new)

        start = tuple(jnp.zeros((tile, half), F32) for _ in range(HEADS))
        done = lax.fori_loop(0, keys, backward, start, unroll=3)
        for h in range(HEADS):
            dq_ref[rows, h * half : (h + 1) * half] = done[h]
        return outer

    lax.fori_loop(0, nodes // tile, tile_step, 0)

    tail = padded - keys * nodes
    kg_ref[keys * nodes :, :] = jnp.zeros((tail, width), BF)
    vg_ref[keys * nodes :, :] = jnp.zeros((tail, width), BF)
    for h in range(HEADS):
        cols = slice(h * half, (h + 1) * half)
        scale = wide(rq_ref[:, h * 128 : (h + 1) * 128])
        unit = q_ref[:, cols]
        slope = dq_ref[:, cols]
        inner = jnp.sum(slope * unit, axis=1, keepdims=True) * (1.0 / half)
        qg_ref[:, cols] = (scale * (slope - unit * inner)).astype(BF)
    mixed = mixf_ref[...].astype(BF)
    mix_ref[...] = mixed
    emb_ref[...] = (matmul(mixed, wo_ref[...]) + self_rows.astype(F32)).astype(BF)

    def pick(b, carry):
        keyed, valued = carry
        at = pl.multiple_of(b * 256, 256)
        rank = jnp.concatenate(
            [rank_ref[place, pl.ds(2 * b, 1), :], rank_ref[place, pl.ds(2 * b + 1, 1), :]], axis=1
        )
        hot = one_hot(sub_iota(ROWCAP, 256) == rank)
        keyed = keyed + matmul(hot, kg_ref[pl.ds(at, 256), :])
        valued = valued + matmul(hot, vg_ref[pl.ds(at, 256), :])
        return keyed, valued

    empty = jnp.zeros((ROWCAP, width), F32)
    keyed, valued = lax.fori_loop(0, padded // 256, pick, (empty, empty), unroll=3)
    hot = one_hot(sub_iota(ROWCAP, nodes) == rank_ref[place, 0:1, 0:nodes])
    queried = matmul(hot, qg_ref[...]).astype(BF)
    total = (
        matmul_right(keyed.astype(BF), wk_ref[...])
        + matmul_right(valued.astype(BF), wv_ref[...])
        + (matmul_right(queried, wq_ref[...]) + matmul(hot, cot_ref[...]))
    ).astype(BF)
    for e in range(4):
        back_ref[e] = total[:, e * 128 : (e + 1) * 128]
    for step, out_ref in enumerate((out0_ref, out1_ref, out2_ref, out3_ref)):
        out_ref[...] = back_ref[(place + step) % 4]


def slots_body(place_ref, sid_ref, row0_ref, row1_ref, row2_ref, row3_ref, flag_ref, out_ref):
    place = place_ref[0]
    buckets = out_ref.shape[0]
    parts = (row0_ref, row1_ref, row2_ref, row3_ref)
    ids = [sid_ref[pl.ds((place + 4 - step) % 4, 1), :] for step in range(4)]
    flag = jnp.broadcast_to(flag_ref[0:1, :], (8, 128))
    group = 4
    span = group * BUCKET

    def step(o, carry):
        slot = sub_iota(span, ROWCAP) + (o * span).astype(F32)
        total = matmul(one_hot(slot == ids[0]), parts[0][...])
        for e in (1, 2, 3):
            total = total + matmul(one_hot(slot == ids[e]), parts[e][...])
        for k in range(group):
            rows = jnp.concatenate([total[k * BUCKET : (k + 1) * BUCKET], flag], axis=0)
            out_ref[o * group + k] = rows.astype(BF)
        return carry

    lax.fori_loop(0, buckets // group, step, 0)


def events_body(index_ref, slots_ref, out_ref, flag_ref):
    flag_ref[...] = jnp.max(slots_ref[:, BUCKET:, :].astype(F32), axis=0)
    events = out_ref.shape[0]
    turns, length = index_ref.shape
    each = length // BUCKET
    for half in range(2):
        base = half * (events // 2)

        def step(t, total):
            places = index_ref[pl.ds(t, 1), :] - base
            hot = one_hot(sub_iota(events // 2, length) == places)
            data = jnp.concatenate(
                [slots_ref[t * each + m, 0:BUCKET, :] for m in range(each)], axis=0
            )
            return total + matmul(hot, data)

        total = lax.fori_loop(0, turns, step, jnp.zeros((events // 2, 128), F32), unroll=2)
        out_ref[base : base + events // 2, :] = total


def refresh_body(
    target_ref, asked_ref, memory_ref, fresh_ref, code_ref, new_ref, out_ref
):
    new_ref[...] = memory_ref[...]
    events = fresh_ref.shape[0]
    owners, table_rows, _ = out_ref.shape
    capacity = table_rows - 8

    def put(i, carry):
        base = pl.multiple_of(i * 16, 16)
        for u in range(16):
            new_ref[pl.ds(target_ref[base + u], 1), :] = fresh_ref[pl.ds(base + u, 1), :]
        return carry

    lax.fori_loop(0, events // 16, put, 0)

    def take_owner(owner, carry):
        base = owner * table_rows

        def take(i, inner):
            first = pl.multiple_of(i * 176, 16)
            for v in range(0, 176, 16):
                at = base + first + v
                rows = [new_ref[pl.ds(asked_ref[at + u], 1), :] for u in range(16)]
                out_ref[owner, pl.ds(pl.multiple_of(first + v, 16), 16), :] = jnp.concatenate(
                    rows, axis=0
                ).astype(BF)
            return inner

        return lax.fori_loop(0, capacity // 176, take, carry)

    lax.fori_loop(0, owners, take_owner, 0)

    def mark(owner, carry):
        code = code_ref[pl.ds(owner, 1), :]
        rows = [code[:, b * 128 : (b + 1) * 128] for b in range(5)] + [jnp.zeros((3, 128), F32)]
        out_ref[owner, capacity:, :] = jnp.concatenate(rows, axis=0).astype(BF)
        return carry

    lax.fori_loop(0, owners, mark, 0, unroll=4)


def take_body(steps, owners, place_ref, index_ref, table_ref, *refs):
    outs, full_ref = refs[: len(steps)], refs[-1]
    full_ref[...] = table_ref[...].astype(F32)
    if len(refs) > len(steps) + 1:
        table_rows = table_ref.shape[0] // owners
        code_ref = refs[len(steps)]
        for o in range(owners):
            first = (o + 1) * table_rows - 8
            code_ref[o : o + 1, :] = jnp.concatenate(
                [full_ref[first + b : first + b + 1, :] for b in range(5)], axis=1
            )
    for step, out_ref in zip(steps, outs):
        count = out_ref.shape[0]
        start = ((place_ref[0] + step) % 4) * count

        def take(i, carry):
            first = pl.multiple_of(i * 128, 128)
            for v in range(0, 128, 32):
                at = start + first + v
                rows = [full_ref[pl.ds(index_ref[at + u], 1), :] for u in range(32)]
                out_ref[pl.ds(pl.multiple_of(first + v, 32), 32), :] = jnp.concatenate(
                    rows, axis=0
                ).astype(BF)
            return carry

        lax.fori_loop(0, count // 128, take, 0)


def add_rows_body(index_ref, rows_ref, out_ref):
    out_ref[...] = jnp.zeros_like(out_ref)

    def add(i, carry):
        at = pl.ds(index_ref[i], 1)
        out_ref[at, :] += rows_ref[pl.ds(i, 1), :]
        return carry

    lax.fori_loop(0, rows_ref.shape[0], add, 0)


def cell_body(
    place_ref,
    arrived_ref,
    code_ref,
    stale_ref,
    part0_ref,
    part1_ref,
    part2_ref,
    part3_ref,
    wx_ref,
    wh_ref,
    bias_ref,
    fresh_ref,
    reset_ref,
    update_ref,
    recall_ref,
    cand_ref,
    input_ref,
    wide_ref,
    in_ref,
):
    place = place_ref[0]
    sources = arrived_ref.shape[0]
    slots = stale_ref.shape[0] // sources
    for step, part_ref in enumerate((part0_ref, part1_ref, part2_ref, part3_ref)):
        in_ref[(place + 4 - step) % 4] = part_ref[...]
    for e in range(4):
        wide_ref[:, e * 128 : (e + 1) * 128] = in_ref[e]
    for s in range(sources):
        input_ref[s * slots : (s + 1) * slots, 0:128] = arrived_ref[s, 0:slots, :]
    input_ref[:, 128:256] = code_ref[...]
    chunk = 256

    def step(c, carry):
        at = pl.multiple_of(c * chunk, chunk)
        inputs = input_ref[pl.ds(at, chunk), :]
        hidden = wide_ref[pl.ds(at, chunk), :]
        stale = stale_ref[pl.ds(at, chunk), :]
        reset = jax.nn.sigmoid(
            matmul(inputs, wx_ref[0]) + matmul(hidden, wh_ref[0]) + bias_ref[0:1, :]
        )
        update = jax.nn.sigmoid(
            matmul(inputs, wx_ref[1]) + matmul(hidden, wh_ref[1]) + bias_ref[1:2, :]
        )
        recall = matmul(hidden, wh_ref[2]) + bias_ref[3:4, :]
        cand = jnp.tanh(matmul(inputs, wx_ref[2]) + bias_ref[2:3, :] + reset * recall)
        fresh = (1.0 - update) * cand + update * stale
        line = lax.broadcasted_iota(I32, (slots, 128), 0).astype(F32)
        live = jnp.concatenate(
            [
                jnp.where(
                    line
                    < arrived_ref[c * (chunk // slots) + k, slots + 8 : slots + 16, :].astype(F32)[
                        3:4
                    ],
                    1.0,
                    0.0,
                )
                for k in range(chunk // slots)
            ],
            axis=0,
        )
        fresh_ref[pl.ds(at, chunk), :] = jnp.where(live > 0.5, fresh, stale)
        reset_ref[pl.ds(at, chunk), :] = reset
        update_ref[pl.ds(at, chunk), :] = update
        recall_ref[pl.ds(at, chunk), :] = recall
        cand_ref[pl.ds(at, chunk), :] = cand
        return carry

    lax.fori_loop(0, stale_ref.shape[0] // chunk, step, 0)


def gates_body(
    grad_ref,
    input_ref,
    wide_ref,
    stale_ref,
    reset_ref,
    update_ref,
    recall_ref,
    cand_ref,
    out_ref,
):
    grad = grad_ref[...]
    reset, update = reset_ref[...], update_ref[...]
    recall, cand = recall_ref[...], cand_ref[...]
    cand_term = grad * (1.0 - update) * (1.0 - cand * cand)
    update_term = grad * (stale_ref[...] - cand) * update * (1.0 - update)
    recall_term = cand_term * reset
    reset_term = cand_term * recall * reset * (1.0 - reset)
    terms = [reset_term, update_term, cand_term, recall_term]
    rounded = [term.astype(BF) for term in terms]
    seen = input_ref.shape[1]
    known = wide_ref.shape[1]
    left = jnp.concatenate(rounded[0:3], axis=1)
    right = jnp.concatenate([rounded[0], rounded[1], rounded[3]], axis=1)
    from_input = matmul_left(input_ref[...], left).astype(BF)
    from_wide = matmul_left(wide_ref[...], right).astype(BF)
    for g in range(3):
        lanes = slice(g * 128, (g + 1) * 128)
        out_ref[g * seen : (g + 1) * seen, :] = from_input[:, lanes]
        out_ref[3 * seen + g * known : 3 * seen + (g + 1) * known, :] = from_wide[:, lanes]
    first = 3 * (seen + known)
    sums = jnp.concatenate(
        [jnp.sum(term, axis=0, keepdims=True) for term in terms] + [jnp.zeros((12, 128), F32)],
        axis=0,
    )
    out_ref[first : first + 16, :] = sums.astype(BF)
    out_ref[first + 16 :, :] = jnp.zeros((out_ref.shape[0] - first - 16, 128), BF)


def weights_body(
    count,
    place_ref,
    wide_ref,
    code_ref,
    mix_ref,
    cot_ref,
    kg_ref,
    vg_ref,
    qg_ref,
    out0_ref,
    out1_ref,
    out2_ref,
    out3_ref,
    block_ref,
):
    place = place_ref[0]
    width = cot_ref.shape[1]
    nodes = cot_ref.shape[0]

    def keep(first, value):
        for e in range(4):
            block_ref[e, first : first + value.shape[0], :] = value[
                :, e * 128 : (e + 1) * 128
            ].astype(BF)

    rows = wide_ref[...]
    keep(0, matmul_left(rows[0:nodes, :], qg_ref[...]))
    keep(width, matmul_left(rows, kg_ref[0:count, :]))
    keep(2 * width, matmul_left(rows, vg_ref[0:count, :]))
    keep(3 * width, matmul_left(code_ref[...], kg_ref[0:count, :]))
    keep(3 * width + 128, matmul_left(mix_ref[...], cot_ref[...]))
    for step, out_ref in enumerate((out0_ref, out1_ref, out2_ref, out3_ref)):
        out_ref[...] = block_ref[(place + step) % 4]


def spread_body(place_ref, b0, b1, b2, b3, query_ref, key_ref, value_ref, time_ref, out_ref, block):
    place = place_ref[0]
    for step, part_ref in enumerate((b0, b1, b2, b3)):
        block[(place + 4 - step) % 4] = part_ref[0 : block.shape[1], :]
    first = 0
    for ref in (query_ref, key_ref, value_ref, time_ref, out_ref):
        for e in range(4):
            ref[:, e * 128 : (e + 1) * 128] = block[e, first : first + ref.shape[0], :].astype(F32)
        first += ref.shape[0]


def exchange(value, axes):
    return lax.all_to_all(value, axes, split_axis=0, concat_axis=0, tiled=True)


def fold_body(parts_ref, out_ref):
    count = parts_ref.shape[0]
    total = parts_ref[0].astype(F32)
    for m in range(1, count):
        total = total + parts_ref[m].astype(F32)
    total = total.astype(BF)
    for m in range(count):
        out_ref[m] = total


def total_body(own_ref, near_ref, far_ref, last_ref, out_ref):
    rows = own_ref.shape[0]
    total = own_ref[...].astype(F32)
    for ref in (near_ref, far_ref, last_ref):
        total = total + ref[...].astype(F32)
    out_ref[0:rows, :] = total.astype(BF)
    out_ref[rows:, :] = jnp.zeros((out_ref.shape[0] - rows, 128), BF)


def split_body(rows_ref, wx_ref, wh_ref, bias_ref):
    first = 0
    for ref in (wx_ref, wh_ref):
        for g in range(3):
            rows = ref.shape[1]
            ref[g] = rows_ref[first : first + rows, :].astype(F32)
            first += rows
    bias_ref[...] = rows_ref[first : first + 16, :].astype(F32)[0:4]


def reduce_mem(value, count):
    parts = value.reshape(count, value.shape[0] // count, value.shape[1])
    arrived = exchange(parts, "mem")
    folded = call(fold_body, shape(*parts.shape, dtype=BF), (arrived,))
    gathered = exchange(folded, "mem")
    return gathered.reshape(value.shape)


def per_device(
    memory,
    ev_rows,
    ev_count,
    ev_feat,
    ev_dt,
    req_rows,
    nbr_slot,
    nbr_dt,
    nbr_len,
    time_freq,
    gru_wx,
    gru_wh,
    gru_bias,
    w_query,
    w_key,
    w_value,
    w_time,
    w_out,
    cotangent,
):
    columns = memory.shape[1]
    rows_dev = memory.shape[0]
    owners, slot_count = ev_rows.shape[1], ev_rows.shape[2]
    capacity = req_rows.shape[2]
    batch, keys = nbr_slot.shape
    nodes = nbr_len.shape[0]
    peers = batch // nodes
    width = columns * peers
    flat_slots = 640
    table_rows = capacity + 8
    picks = 2176

    packed = call(
        pack_body,
        shape(owners, slot_count + 16, 128, dtype=BF),
        (ev_feat[0], req_rows[0], jnp.transpose(nbr_slot), ev_rows[0], ev_dt[0], ev_count),
        [pltpu.VMEM((owners, flat_slots), I32)],
    )
    arrived = exchange(packed, "mem")

    line = arrived[:, slot_count + 10, :].astype(I32)
    targets = (line[:, :slot_count] * 64 + line[:, slot_count : 2 * slot_count]).reshape(-1)
    deltas = line[:, 2 * slot_count : 3 * slot_count] * 32 + line[:, 3 * slot_count :]
    live_counts = arrived[:, slot_count + 11, 0:1].astype(I32)
    live_mask = (jnp.arange(slot_count, dtype=I32)[None, :] < live_counts).reshape(-1)
    asked = (
        arrived[:, slot_count : slot_count + 5, :].astype(I32) * 64
        + arrived[:, slot_count + 5 : slot_count + 10, :].astype(I32)
    ).reshape(owners, flat_slots)
    asked = jnp.minimum(asked[:, :table_rows], rows_dev - 1)

    place = lax.axis_index("emb").astype(I32).reshape(1)
    total_events = owners * slot_count
    stale_rows, stale_half = call(
        stale_body,
        (shape(total_events, columns), shape(total_events, columns, dtype=BF)),
        (targets, memory),
        scalars=1,
    )
    wide_parts = [stale_half] + [send(stale_half, step, peers) for step in (1, 2, 3)]
    codes_event = time_code(deltas.reshape(-1), time_freq)
    codes, events, ranks = call(
        functools.partial(route_body, slot_count),
        (
            jax.ShapeDtypeStruct((owners, flat_slots), F32),
            jax.ShapeDtypeStruct((owners, flat_slots), F32),
            jax.ShapeDtypeStruct((owners, flat_slots), F32),
        ),
        (arrived,),
        [pltpu.VMEM((owners, flat_slots), F32)],
    )
    index = call(compact_body, shape(8, owners // 8 * BUCKET), (events, ranks))
    fresh_rows, reset, update, recall, cand, inputs, hidden_wide = call(
        cell_body,
        (shape(total_events, columns),) * 5
        + (shape(total_events, 256, dtype=BF), shape(total_events, width, dtype=BF)),
        (place, arrived, codes_event, stale_rows, *wide_parts, gru_wx, gru_wh, gru_bias),
        [pltpu.VMEM((peers, total_events, columns), BF)],
        scalars=1,
    )
    new_memory, outgoing = call(
        refresh_body,
        (shape(rows_dev, columns), shape(owners, table_rows, columns, dtype=BF)),
        (
            targets,
            asked.reshape(-1),
            memory,
            fresh_rows,
            codes,
        ),
        scalars=2,
    )
    fetched = exchange(outgoing, "mem")

    ordered = jnp.transpose(nbr_slot.reshape(peers, nodes, keys), (0, 2, 1)).reshape(peers, -1)
    count = keys * nodes
    row_index = jnp.pad(ordered + 8 * (ordered // capacity), ((0, 0), (0, picks - count)))
    table = fetched.reshape(-1, columns)
    part = shape(picks, columns, dtype=BF)
    row_index = row_index.reshape(-1)

    def taken(steps, extra=()):
        return call(
            functools.partial(take_body, steps, owners),
            (part,) * len(steps) + extra,
            (place, row_index, table),
            [pltpu.VMEM(table.shape, F32)],
            scalars=2,
        )

    near, far, slot_codes = taken((1, 2), (shape(owners, flat_slots),))
    near = send(near, 1, peers)
    far = send(far, 2, peers)
    last, own = taken((3, 0))
    last = send(last, 3, peers)

    slots_in = jnp.pad(ordered, ((0, 0), (0, 24 * 128 - count)), constant_values=-1)
    slots_in = slots_in.reshape(peers, 24, 128)
    pick_rank, slot_list, flag = call(
        functools.partial(picks_body, capacity),
        (
            jax.ShapeDtypeStruct((peers, 24, 128), F32),
            jax.ShapeDtypeStruct((peers, ROWCAP), F32),
            jax.ShapeDtypeStruct((8, 128), F32),
        ),
        (slot_codes, slots_in),
        [pltpu.VMEM((peers, 24, 128), F32)],
    )

    lengths = jnp.broadcast_to(nbr_len.astype(F32)[:, None], (nodes, 128))
    codes_in = time_code(jnp.transpose(nbr_dt).reshape(-1), time_freq)
    padded = 2304
    embedding, mixed, key_grad, value_grad, query_grad, rows_wide, *compact_rows = call(
        functools.partial(attend_body, keys),
        (
            jax.ShapeDtypeStruct((nodes, width), BF),
            jax.ShapeDtypeStruct((nodes, width), BF),
            jax.ShapeDtypeStruct((padded, width), BF),
            jax.ShapeDtypeStruct((padded, width), BF),
            jax.ShapeDtypeStruct((nodes, width), BF),
            jax.ShapeDtypeStruct((count, width), BF),
        )
        + (shape(ROWCAP, columns, dtype=BF),) * 4,
        (
            place,
            own,
            near,
            far,
            last,
            codes_in,
            lengths,
            cotangent,
            pick_rank,
            w_query,
            w_key,
            w_value,
            w_time,
            w_out,
        ),
        [
            pltpu.VMEM((count, width), BF),
            pltpu.VMEM((count, width), BF),
            pltpu.VMEM((nodes, width), F32),
            pltpu.VMEM((nodes, width), F32),
            pltpu.VMEM((nodes, 256), F32),
            pltpu.VMEM((count, 256), F32),
            pltpu.VMEM((count, 256), F32),
            pltpu.VMEM((count, 256), F32),
            pltpu.VMEM((count, 256), F32),
            pltpu.VMEM((nodes, 256), F32),
            pltpu.VMEM((nodes, 256), F32),
            pltpu.VMEM((nodes, width), F32),
            pltpu.VMEM((nodes, width), F32),
            pltpu.VMEM((peers, count, columns), BF),
            pltpu.VMEM((peers, ROWCAP, columns), BF),
        ],
        scalars=1,
        flops=8 * 10**9,
    )

    returned_rows = compact_rows[:1]
    for step in (1, 2, 3):
        returned_rows.append(send(compact_rows[step], step, peers))
    slot_sums = call(
        slots_body,
        shape(owners, BUCKET + 8, columns, dtype=BF),
        (place, slot_list, *returned_rows, flag),
        scalars=1,
    )
    returned = exchange(slot_sums, "mem")
    sparse_grad, flags = call(
        events_body, (shape(total_events, columns), shape(8, 128)), (index, returned)
    )
    spilled = flags[0, 0] > 0.0

    def dense_grad(_):
        key_rows, value_rows = key_grad[:count], value_grad[:count]
        grad = matmul_right(key_rows, w_key) + matmul_right(value_rows, w_value)
        own = matmul_right(query_grad, w_query) + cotangent.astype(F32)
        grad = grad.at[:nodes].add(own).astype(BF)
        parts = jnp.transpose(grad.reshape(count, peers, columns), (1, 0, 2))
        parts = exchange(parts, "emb").reshape(-1, columns).astype(F32)
        sums = call(
            add_rows_body,
            shape(owners * capacity, columns),
            (ordered.reshape(-1), parts),
            scalars=1,
        )
        back = exchange(sums.astype(BF).reshape(owners, capacity, columns), "mem")
        table = call(
            add_rows_body,
            shape(rows_dev, columns),
            (asked[:, :capacity].reshape(-1), back.reshape(-1, columns).astype(F32)),
            scalars=1,
        )
        return jnp.where(live_mask[:, None], table[targets], 0.0)

    grad_fresh = lax.cond(spilled, dense_grad, lambda kept: kept, sparse_grad)

    total_weight = 3 * width + 128 + width
    shard = owners * 80
    weight_parts = call(
        functools.partial(weights_body, count),
        (shape(total_weight, columns, dtype=BF),) * 4,
        (
            place,
            rows_wide,
            codes_in,
            mixed,
            cotangent,
            key_grad,
            value_grad,
            query_grad,
        ),
        [pltpu.VMEM((peers, total_weight, columns), BF)],
        scalars=1,
        flops=2 * 10**9,
    )
    moved = [weight_parts[0]]
    for step in (1, 2, 3):
        moved.append(send(weight_parts[step], step, peers))
    weight_sum = call(total_body, shape(shard, columns, dtype=BF), tuple(moved))
    weight_sum = reduce_mem(weight_sum, owners)[:total_weight]
    spread_parts = []
    for step in (1, 2, 3):
        spread_parts.append(send(weight_sum, step, peers))
    grad_query, grad_key, grad_value, grad_time, grad_out = call(
        spread_body,
        (
            shape(width, width),
            shape(width, width),
            shape(width, width),
            shape(128, width),
            shape(width, width),
        ),
        (place, weight_sum, *spread_parts),
        [pltpu.VMEM((peers, total_weight, columns), BF)],
        scalars=1,
    )

    gate_rows = call(
        gates_body,
        shape(shard, columns, dtype=BF),
        (grad_fresh, inputs, hidden_wide, stale_rows, reset, update, recall, cand),
    )
    gate_rows = reduce_mem(gate_rows, owners)
    grad_wx, grad_wh, grad_bias = call(
        split_body,
        (shape(*gru_wx.shape), shape(*gru_wh.shape), shape(*gru_bias.shape)),
        (gate_rows,),
    )
    return (
        new_memory,
        embedding,
        grad_wx,
        grad_wh,
        grad_bias,
        grad_query,
        grad_key,
        grad_value,
        grad_time,
        grad_out,
    )


def solution(mesh):
    in_specs = (
        P("mem", "emb"),
        P("mem", None, None),
        P("mem", None),
        P("mem", None, None, None),
        P("mem", None, None),
        P("mem", None, None),
        P("mem", None),
        P(("mem", "emb"), None),
        P(("mem", "emb")),
        P(),
        P(None, None, "emb"),
        P(None, None, "emb"),
        P(None, "emb"),
        P(),
        P(),
        P(),
        P(),
        P(),
        P(("mem", "emb"), None),
    )
    out_specs = (
        P("mem", "emb"),
        P(("mem", "emb"), None),
        P(None, None, "emb"),
        P(None, None, "emb"),
        P(None, "emb"),
        P(),
        P(),
        P(),
        P(),
        P(),
    )

    return jax.shard_map(
        per_device, mesh=mesh, in_specs=in_specs, out_specs=out_specs, check_vma=False
    )
```

```python
import functools
import math

import jax
import jax.numpy as jnp
from jax import lax
from jax.experimental import pallas as pl
from jax.experimental.pallas import tpu as pltpu
from jax.sharding import PartitionSpec as P


HEADS = 2
EPSILON = 1e-06
BUCKET = 160
ROWCAP = 384
SPILL = 200.0

BF = jnp.bfloat16
F32 = jnp.float32
I32 = jnp.int32


def matmul(left_side, right_side):
    return jnp.dot(left_side, right_side, preferred_element_type=F32)


def matmul_left(left_side, right_side):
    return lax.dot_general(
        left_side, right_side, (((0,), (0,)), ((), ())), preferred_element_type=F32
    )


def matmul_right(left_side, right_side):
    return lax.dot_general(
        left_side, right_side, (((1,), (1,)), ((), ())), preferred_element_type=F32
    )


def time_code(time_delta, time_freq):
    return jnp.cos(time_delta.astype(F32)[..., None] * time_freq).astype(BF)


def one_hot(condition):
    return jnp.where(condition, 1.0, 0.0).astype(BF)


def sub_iota(rows, lanes):
    return lax.broadcasted_iota(I32, (rows, lanes), 0).astype(F32)


def hot_rows(rows, index):
    blocks = []
    for first in range(0, rows, 256):
        size = min(256, rows - first)
        line = lax.broadcasted_iota(I32, (size, index.shape[1]), 0).astype(F32).astype(BF)
        same = line == (index - float(first)).astype(BF)
        blocks.append(jnp.where(same, jnp.ones((), BF), jnp.zeros((), BF)))
    return blocks[0] if len(blocks) == 1 else jnp.concatenate(blocks, axis=0)


def call(body, out_shape, args, scratch=(), scalars=0, flops=10**8):
    spaces = [pltpu.SMEM] * scalars + [pltpu.VMEM] * (len(args) - scalars)
    return pl.pallas_call(
        body,
        out_shape=out_shape,
        in_specs=[pl.BlockSpec(memory_space=space) for space in spaces],
        out_specs=jax.tree.map(lambda _: pl.BlockSpec(memory_space=pltpu.VMEM), out_shape),
        scratch_shapes=list(scratch),
        cost_estimate=pl.CostEstimate(flops=flops, transcendentals=0, bytes_accessed=10**6),
        compiler_params=pltpu.CompilerParams(vmem_limit_bytes=56 << 20),
    )(*args)


def shape(*dims, dtype=F32):
    return jax.ShapeDtypeStruct(dims, dtype)


def send(value, step, peers):
    return lax.ppermute(value, "emb", [(e, (e + step) % peers) for e in range(peers)])


def pack_body(feat_ref, req_ref, slot_ref, row_ref, dt_ref, count_ref, out_ref, req_scr):
    owners, slots, _ = feat_ref.shape
    capacity = req_ref.shape[1]
    width = req_scr.shape[1]
    req_scr[:, 0:capacity] = req_ref[...]
    slot = slot_ref[...].astype(F32)
    bucket = jnp.floor((slot + 0.5) * (1.0 / capacity))
    inside = slot - bucket * capacity + 1.0
    counts = count_ref[...].astype(F32)
    owner_lane = lax.broadcasted_iota(I32, counts.shape, 1)
    lane = lax.broadcasted_iota(I32, (1, width), 1).astype(F32)

    def step(o, carry):
        mine = jnp.where(bucket == o.astype(F32), inside, 0.0)
        filled = jnp.max(jnp.max(mine, axis=0, keepdims=True), axis=1, keepdims=True)
        asked = req_scr[pl.ds(o, 1), :]
        used = lane < filled
        high = jnp.where(used, (asked >> 6).astype(F32), 64.0)
        low = jnp.where(used, (asked & 63).astype(F32), 0.0)
        row = row_ref[pl.ds(o, 1), :]
        delta = dt_ref[pl.ds(o, 1), :]
        line = jnp.concatenate([row >> 6, row & 63, delta >> 5, delta & 31], axis=1).astype(F32)
        count = jnp.sum(jnp.where(owner_lane == o, counts, 0.0), axis=1, keepdims=True)
        count = jnp.broadcast_to(count, (1, 128))
        block = jnp.concatenate(
            [high[:, b * 128 : (b + 1) * 128] for b in range(5)]
            + [low[:, b * 128 : (b + 1) * 128] for b in range(5)]
            + [line, count, jnp.zeros((4, 128), F32)],
            axis=0,
        )
        out_ref[o, 0:slots, :] = feat_ref[o]
        out_ref[o, slots:, :] = block.astype(BF)
        return carry

    lax.fori_loop(0, owners, step, 0, unroll=4)


def stale_body(target_ref, memory_ref, out_ref, half_ref):
    def take(i, carry):
        first = pl.multiple_of(i * 32, 32)
        rows = [memory_ref[pl.ds(target_ref[first + u], 1), :] for u in range(32)]
        rows = jnp.concatenate(rows, axis=0)
        out_ref[pl.ds(first, 32), :] = rows
        half_ref[pl.ds(first, 32), :] = rows.astype(BF)
        return carry

    lax.fori_loop(0, out_ref.shape[0] // 32, take, 0)


def route_body(feat_rows, msg_ref, code_ref, event_ref, rel_ref, rank_ref):
    sources = msg_ref.shape[0]
    slots = feat_rows
    width = rel_ref.shape[1]
    blocks = width // 128

    def table_step(s, table):
        block = msg_ref[s].astype(F32)
        high = block[slots + 10 : slots + 11, 0:slots]
        low = block[slots + 10 : slots + 11, slots : 2 * slots]
        count = block[slots + 11 : slots + 12, 0:slots]
        lane = lax.broadcasted_iota(I32, (1, slots), 1).astype(F32)
        live = lane < count
        high_hot = one_hot(sub_iota(64, slots) == high)
        low_hit = (sub_iota(64, slots) == low) & live
        first = jnp.where(low_hit, s.astype(F32) + 1.0, 0.0).astype(BF)
        second = jnp.where(low_hit, lane, 0.0).astype(BF)
        return table + matmul_right(jnp.concatenate([first, second], axis=0), high_hot)

    table = lax.fori_loop(
        0, sources, table_step, jnp.zeros((128, 64), F32), unroll=4
    ).astype(BF)

    def flat(s, first_row):
        block = msg_ref[s].astype(F32)
        return jnp.concatenate(
            [block[first_row + b : first_row + b + 1, :] for b in range(blocks)], axis=1
        )

    def find_step(s, carry):
        high = flat(s, slots)
        low = flat(s, slots + 5)
        high_hot = one_hot(sub_iota(64, width) == high)
        low_hit = sub_iota(64, width) == low
        found = matmul(table, high_hot)
        event_ref[pl.ds(s, 1), :] = jnp.sum(
            jnp.where(low_hit, found[0:64], 0.0), axis=0, keepdims=True
        )
        rank_ref[pl.ds(s, 1), :] = jnp.sum(
            jnp.where(low_hit, found[64:128], 0.0), axis=0, keepdims=True
        )
        return carry

    lax.fori_loop(0, sources, find_step, 0, unroll=2)
    first = event_ref[...]
    relevant = first > 0.0
    before = one_hot(
        lax.broadcasted_iota(I32, (width, width), 0) < lax.broadcasted_iota(I32, (width, width), 1)
    )
    rank = matmul(one_hot(relevant), before)
    event = (first - 1.0) * slots + rank_ref[...]
    code_ref[...] = jnp.where(
        relevant, jnp.where(rank < BUCKET, rank + 1.0, SPILL), 0.0
    )
    event_ref[...] = jnp.where(relevant, event, -1.0)
    rel_ref[...] = jnp.where(relevant, rank, -1.0)


def compact_body(event_ref, rel_ref, index_ref):
    _, width = rel_ref.shape
    turns, length = index_ref.shape
    each = length // BUCKET

    def step(t, carry):
        lines = []
        for m in range(each):
            rank = rel_ref[pl.ds(t * each + m, 1), :]
            event = event_ref[pl.ds(t * each + m, 1), :]
            hot = one_hot(sub_iota(BUCKET, width) == rank)
            high = jnp.floor(event * (1.0 / 32.0))
            low = event - high * 32.0
            have = jnp.where(rank >= 0.0, 1.0, 0.0)
            row = lax.broadcasted_iota(I32, (8, width), 0)
            digits = jnp.where(
                row == 0,
                high * have,
                jnp.where(row == 1, low * have, jnp.where(row == 2, have, 0.0)),
            ).astype(BF)
            got = matmul_right(digits, hot)
            lines.append(jnp.where(got[2:3] > 0.5, got[0:1] * 32.0 + got[1:2], -1.0))
        index_ref[pl.ds(t, 1), :] = jnp.concatenate(lines, axis=1)
        return carry

    lax.fori_loop(0, turns, step, 0)


def picks_body(capacity, code_ref, slot_ref, rank_ref, sid_ref, flag_ref, got_ref):
    owners, width = code_ref.shape
    peers, rows, lanes = slot_ref.shape
    fine = 16
    coarse = width // fine
    codes = code_ref[...].astype(BF)
    spot = lax.broadcasted_iota(I32, (width, 128), 0)
    column = lax.broadcasted_iota(I32, (width, 128), 1)
    table = jnp.concatenate(
        [matmul(codes, one_hot(spot == column * fine + low)) for low in range(fine)], axis=0
    ).astype(BF)[:, 0:coarse]

    def pair(ref, peer, row):
        return jnp.concatenate(
            [ref[peer, pl.ds(row, 1), :], ref[peer, pl.ds(row + 1, 1), :]], axis=1
        )

    def place_of(slot):
        owner = jnp.floor((slot + 0.5) * (1.0 / capacity))
        return owner, slot - owner * capacity

    def lookup(step, carry):
        peer = step // 9
        row = (step % 9) * 2
        slot = pair(slot_ref, peer, row).astype(F32)
        owner, inside = place_of(slot)
        high = jnp.floor(inside * (1.0 / fine))
        found = matmul(table, one_hot(sub_iota(coarse, 2 * lanes) == high))
        mine = sub_iota(fine * owners, 2 * lanes) == (inside - high * fine) * owners + owner
        got = jnp.sum(jnp.where(mine, found, 0.0), axis=0, keepdims=True)
        got = jnp.where(slot >= 0.0, got, 0.0)
        got_ref[peer, pl.ds(row, 1), :] = got[:, 0:lanes]
        got_ref[peer, pl.ds(row + 1, 1), :] = got[:, lanes:]
        return carry

    got_ref[:, 16:24, :] = jnp.zeros((peers, 8, lanes), F32)
    lax.fori_loop(0, peers * 9, lookup, 0, unroll=4)
    lane_before = one_hot(
        lax.broadcasted_iota(I32, (lanes, lanes), 0) < lax.broadcasted_iota(I32, (lanes, lanes), 1)
    )
    row_before = one_hot(
        lax.broadcasted_iota(I32, (rows, rows), 1) < lax.broadcasted_iota(I32, (rows, rows), 0)
    )
    ones = jnp.ones((lanes, lanes), BF)

    def order(peer, flag):
        got = got_ref[peer]
        relevant = got > 0.0
        hot = one_hot(relevant)
        rank = matmul(hot, lane_before) + matmul(row_before, matmul(hot, ones).astype(BF))
        rank = jnp.where(relevant, rank, -1.0)
        rank_ref[peer] = rank
        bad = jnp.where((got >= SPILL) | (rank >= ROWCAP), 1.0, 0.0)
        return jnp.maximum(flag, jnp.max(bad, axis=(0, 1), keepdims=True))

    flag_ref[...] = lax.fori_loop(0, peers, order, jnp.zeros((8, lanes), F32))

    def collect(peer, carry):
        def gather(step, total):
            row = step * 2
            owner, _ = place_of(pair(slot_ref, peer, row).astype(F32))
            rank = pair(rank_ref, peer, row)
            code = pair(got_ref, peer, row)
            have = jnp.where(rank >= 0.0, 1.0, 0.0)
            hot = hot_rows(ROWCAP, rank)
            line = lax.broadcasted_iota(I32, (128, 2 * lanes), 0)
            digits = jnp.where(
                line == 0,
                owner * have,
                jnp.where(line == 1, (code - 1.0) * have, jnp.where(line == 2, have, 0.0)),
            ).astype(BF)
            return total + matmul_right(hot, digits)

        total = lax.fori_loop(0, 9, gather, jnp.zeros((ROWCAP, 128), F32), unroll=3)
        total = jnp.transpose(total)
        sid_ref[pl.ds(peer, 1), :] = jnp.where(
            total[2:3] > 0.5, total[0:1] * BUCKET + total[1:2], -1.0
        )
        return carry

    lax.fori_loop(0, peers, collect, 0)


def attend_body(
    keys,
    place_ref,
    part0_ref,
    part1_ref,
    part2_ref,
    part3_ref,
    code_ref,
    mask_ref,
    cot_ref,
    rank_ref,
    wq_ref,
    wk_ref,
    wv_ref,
    wt_ref,
    wo_ref,
    emb_ref,
    mix_ref,
    kg_ref,
    vg_ref,
    qg_ref,
    wide_ref,
    out0_ref,
    out1_ref,
    out2_ref,
    out3_ref,
    k_ref,
    v_ref,
    q_ref,
    g_ref,
    rq_ref,
    e_ref,
    r_ref,
    a_ref,
    d_ref,
    den_ref,
    dp_ref,
    mixf_ref,
    dq_ref,
    in_ref,
    back_ref,
):
    place = place_ref[0]
    nodes = cot_ref.shape[0]
    width = cot_ref.shape[1]
    half = width // HEADS
    chunk = 11 * nodes
    padded = kg_ref.shape[0]

    for step, part_ref in enumerate((part0_ref, part1_ref, part2_ref, part3_ref)):
        in_ref[(place + 4 - step) % 4] = part_ref[0 : keys * nodes, :]
    for e in range(4):
        wide_ref[:, e * 128 : (e + 1) * 128] = in_ref[e]

    def row_block(first, count):
        return wide_ref[pl.ds(first, count), :]

    def project(c, carry):
        at = pl.multiple_of(c * chunk, chunk)
        block = row_block(at, chunk)
        k_ref[pl.ds(at, chunk), :] = (
            matmul(block, wk_ref[...]) + matmul(code_ref[pl.ds(at, chunk), :], wt_ref[...])
        ).astype(BF)
        v_ref[pl.ds(at, chunk), :] = matmul(block, wv_ref[...]).astype(BF)
        return carry

    lax.fori_loop(0, keys // 11, project, 0)
    self_rows = row_block(0, nodes)
    query = matmul(self_rows, wq_ref[...]).astype(BF).astype(F32)
    g_ref[...] = matmul_right(cot_ref[...], wo_ref[...])
    for h in range(HEADS):
        part = query[:, h * half : (h + 1) * half]
        scale = lax.rsqrt(jnp.sum(part * part, axis=1, keepdims=True) * (1.0 / half) + EPSILON)
        rq_ref[:, h * 128 : (h + 1) * 128] = jnp.broadcast_to(scale, (nodes, 128))
        q_ref[:, h * half : (h + 1) * half] = part * scale

    tile = 16
    inv_root = 1.0 / math.sqrt(half)

    def wide(x):
        return jnp.concatenate([x, x], axis=1)

    def tile_step(t, outer):
        lo = pl.multiple_of(t * tile, tile)
        rows = pl.ds(lo, tile)

        def forward(j, carry):
            at = pl.multiple_of(j * nodes + lo, tile)
            key = k_ref[pl.ds(at, tile), :].astype(F32)
            value = v_ref[pl.ds(at, tile), :].astype(F32)
            valid = jnp.where(j.astype(F32) <= mask_ref[rows, :], 1.0, 0.0)
            new = []
            for h in range(HEADS):
                den, dp, mixed = carry[h]
                cols = slice(h * half, (h + 1) * half)
                kh, vh = key[:, cols], value[:, cols]
                qh = q_ref[rows, cols]
                gh = g_ref[rows, cols]
                square = jnp.sum(kh * kh, axis=1, keepdims=True)
                inner = jnp.sum(qh * kh, axis=1, keepdims=True)
                toward = jnp.sum(gh * vh, axis=1, keepdims=True)
                square = jnp.broadcast_to(square, (tile, 128))
                inner = jnp.broadcast_to(inner, (tile, 128))
                toward = jnp.broadcast_to(toward, (tile, 128))
                scale = lax.rsqrt(square * (1.0 / half) + EPSILON)
                weight = jnp.exp(scale * inner * inv_root) * valid
                lanes = slice(h * 128, (h + 1) * 128)
                e_ref[pl.ds(at, tile), lanes] = weight
                r_ref[pl.ds(at, tile), lanes] = scale
                a_ref[pl.ds(at, tile), lanes] = inner
                d_ref[pl.ds(at, tile), lanes] = toward
                new.append((den + weight, dp + weight * toward, mixed + wide(weight) * vh))
            return tuple(new)

        zero = jnp.zeros((tile, 128), F32)
        start = tuple((zero, zero, jnp.zeros((tile, half), F32)) for _ in range(HEADS))
        done = lax.fori_loop(0, keys, forward, start, unroll=3)
        for h in range(HEADS):
            den, dp, mixed = done[h]
            inverse = 1.0 / den
            lanes = slice(h * 128, (h + 1) * 128)
            den_ref[rows, lanes] = inverse
            dp_ref[rows, lanes] = dp * inverse
            mixf_ref[rows, h * half : (h + 1) * half] = mixed * wide(inverse)

        def backward(j, carry):
            at = pl.multiple_of(j * nodes + lo, tile)
            key = k_ref[pl.ds(at, tile), :].astype(F32)
            new = []
            for h in range(HEADS):
                cols = slice(h * half, (h + 1) * half)
                lanes = slice(h * 128, (h + 1) * 128)
                kh = key[:, cols]
                qh = q_ref[rows, cols]
                gh = g_ref[rows, cols]
                weight = e_ref[pl.ds(at, tile), lanes] * den_ref[rows, lanes]
                scale = r_ref[pl.ds(at, tile), lanes]
                inner = a_ref[pl.ds(at, tile), lanes]
                toward = d_ref[pl.ds(at, tile), lanes]
                slope = weight * (toward - dp_ref[rows, lanes]) * inv_root
                along = slope * scale
                against = along * scale * scale * inner * (1.0 / half)
                along = wide(along)
                kg_ref[pl.ds(at, tile), cols] = (along * qh - wide(against) * kh).astype(BF)
                vg_ref[pl.ds(at, tile), cols] = (wide(weight) * gh).astype(BF)
                new.append(carry[h] + along * kh)
            return tuple(new)

        start = tuple(jnp.zeros((tile, half), F32) for _ in range(HEADS))
        done = lax.fori_loop(0, keys, backward, start, unroll=3)
        for h in range(HEADS):
            dq_ref[rows, h * half : (h + 1) * half] = done[h]
        return outer

    lax.fori_loop(0, nodes // tile, tile_step, 0)

    tail = padded - keys * nodes
    kg_ref[keys * nodes :, :] = jnp.zeros((tail, width), BF)
    vg_ref[keys * nodes :, :] = jnp.zeros((tail, width), BF)
    for h in range(HEADS):
        cols = slice(h * half, (h + 1) * half)
        scale = wide(rq_ref[:, h * 128 : (h + 1) * 128])
        unit = q_ref[:, cols]
        slope = dq_ref[:, cols]
        inner = jnp.sum(slope * unit, axis=1, keepdims=True) * (1.0 / half)
        qg_ref[:, cols] = (scale * (slope - unit * inner)).astype(BF)
    mixed = mixf_ref[...].astype(BF)
    mix_ref[...] = mixed
    emb_ref[...] = (matmul(mixed, wo_ref[...]) + self_rows.astype(F32)).astype(BF)

    def pick(b, carry):
        keyed, valued = carry
        at = pl.multiple_of(b * 256, 256)
        rank = jnp.concatenate(
            [rank_ref[place, pl.ds(2 * b, 1), :], rank_ref[place, pl.ds(2 * b + 1, 1), :]], axis=1
        )
        hot = hot_rows(ROWCAP, rank)
        keyed = keyed + matmul(hot, kg_ref[pl.ds(at, 256), :])
        valued = valued + matmul(hot, vg_ref[pl.ds(at, 256), :])
        return keyed, valued

    empty = jnp.zeros((ROWCAP, width), F32)
    keyed, valued = lax.fori_loop(0, padded // 256, pick, (empty, empty), unroll=3)
    hot = one_hot(sub_iota(ROWCAP, nodes) == rank_ref[place, 0:1, 0:nodes])
    queried = matmul(hot, qg_ref[...]).astype(BF)
    total = (
        matmul_right(keyed.astype(BF), wk_ref[...])
        + matmul_right(valued.astype(BF), wv_ref[...])
        + (matmul_right(queried, wq_ref[...]) + matmul(hot, cot_ref[...]))
    ).astype(BF)
    for e in range(4):
        back_ref[e] = total[:, e * 128 : (e + 1) * 128]
    for step, out_ref in enumerate((out0_ref, out1_ref, out2_ref, out3_ref)):
        out_ref[...] = back_ref[(place + step) % 4]


def slots_body(place_ref, sid_ref, row0_ref, row1_ref, row2_ref, row3_ref, flag_ref, out_ref):
    place = place_ref[0]
    buckets = out_ref.shape[0]
    parts = (row0_ref, row1_ref, row2_ref, row3_ref)
    ids = [sid_ref[pl.ds((place + 4 - step) % 4, 1), :] for step in range(4)]
    flag = jnp.broadcast_to(flag_ref[0:1, :], (8, 128))
    group = 4

    def step(o, carry):
        total = None
        for e in range(4):
            hot = jnp.concatenate(
                [
                    hot_rows(BUCKET, ids[e] - ((o * group + k) * BUCKET).astype(F32))
                    for k in range(group)
                ],
                axis=0,
            )
            part = matmul(hot, parts[e][...])
            total = part if total is None else total + part
        for k in range(group):
            rows = jnp.concatenate([total[k * BUCKET : (k + 1) * BUCKET], flag], axis=0)
            out_ref[o * group + k] = rows.astype(BF)
        return carry

    lax.fori_loop(0, buckets // group, step, 0)


def events_body(index_ref, slots_ref, out_ref, flag_ref):
    flag_ref[...] = jnp.max(slots_ref[:, BUCKET:, :].astype(F32), axis=0)
    events = out_ref.shape[0]
    turns, length = index_ref.shape
    each = length // BUCKET

    def part(half, carry):
        base = pl.multiple_of(half * (events // 2), events // 2)

        def step(t, total):
            hot = hot_rows(events // 2, index_ref[pl.ds(t, 1), :] - base.astype(F32))
            data = jnp.concatenate(
                [slots_ref[t * each + m, 0:BUCKET, :] for m in range(each)], axis=0
            )
            return total + matmul(hot, data)

        total = lax.fori_loop(0, turns, step, jnp.zeros((events // 2, 128), F32), unroll=2)
        out_ref[pl.ds(base, events // 2), :] = total
        return carry

    lax.fori_loop(0, 2, part, 0)


def refresh_body(
    target_ref, asked_ref, memory_ref, fresh_ref, code_ref, new_ref, out_ref
):
    new_ref[...] = memory_ref[...]
    events = fresh_ref.shape[0]
    owners, table_rows, _ = out_ref.shape
    capacity = table_rows - 8

    def put(i, carry):
        base = pl.multiple_of(i * 16, 16)
        for u in range(16):
            new_ref[pl.ds(target_ref[base + u], 1), :] = fresh_ref[pl.ds(base + u, 1), :]
        return carry

    lax.fori_loop(0, events // 16, put, 0)

    def take_owner(owner, carry):
        base = owner * table_rows

        def take(i, inner):
            first = pl.multiple_of(i * 176, 16)
            for v in range(0, 176, 16):
                at = base + first + v
                rows = [new_ref[pl.ds(asked_ref[at + u], 1), :] for u in range(16)]
                out_ref[owner, pl.ds(pl.multiple_of(first + v, 16), 16), :] = jnp.concatenate(
                    rows, axis=0
                ).astype(BF)
            return inner

        return lax.fori_loop(0, capacity // 176, take, carry)

    lax.fori_loop(0, owners, take_owner, 0)

    def mark(owner, carry):
        code = code_ref[pl.ds(owner, 1), :]
        rows = [code[:, b * 128 : (b + 1) * 128] for b in range(5)] + [jnp.zeros((3, 128), F32)]
        out_ref[owner, capacity:, :] = jnp.concatenate(rows, axis=0).astype(BF)
        return carry

    lax.fori_loop(0, owners, mark, 0, unroll=4)


def take_body(steps, owners, place_ref, index_ref, table_ref, *refs):
    outs, full_ref = refs[: len(steps)], refs[-1]
    full_ref[...] = table_ref[...].astype(F32)
    if len(refs) > len(steps) + 1:
        table_rows = table_ref.shape[0] // owners
        code_ref = refs[len(steps)]
        for o in range(owners):
            first = (o + 1) * table_rows - 8
            code_ref[o : o + 1, :] = jnp.concatenate(
                [full_ref[first + b : first + b + 1, :] for b in range(5)], axis=1
            )
    for step, out_ref in zip(steps, outs):
        count = out_ref.shape[0]
        start = ((place_ref[0] + step) % 4) * count

        def take(i, carry):
            first = pl.multiple_of(i * 64, 64)
            for v in range(0, 64, 32):
                at = start + first + v
                rows = [full_ref[pl.ds(index_ref[at + u], 1), :] for u in range(32)]
                out_ref[pl.ds(pl.multiple_of(first + v, 32), 32), :] = jnp.concatenate(
                    rows, axis=0
                ).astype(BF)
            return carry

        lax.fori_loop(0, count // 64, take, 0)


def add_rows_body(index_ref, rows_ref, out_ref):
    out_ref[...] = jnp.zeros_like(out_ref)

    def add(i, carry):
        at = pl.ds(index_ref[i], 1)
        out_ref[at, :] += rows_ref[pl.ds(i, 1), :]
        return carry

    lax.fori_loop(0, rows_ref.shape[0], add, 0)


def cell_body(
    place_ref,
    arrived_ref,
    code_ref,
    stale_ref,
    part0_ref,
    part1_ref,
    part2_ref,
    part3_ref,
    wx_ref,
    wh_ref,
    bias_ref,
    fresh_ref,
    reset_ref,
    update_ref,
    recall_ref,
    cand_ref,
    input_ref,
    wide_ref,
    in_ref,
):
    place = place_ref[0]
    sources = arrived_ref.shape[0]
    slots = stale_ref.shape[0] // sources
    for step, part_ref in enumerate((part0_ref, part1_ref, part2_ref, part3_ref)):
        in_ref[(place + 4 - step) % 4] = part_ref[...]
    for e in range(4):
        wide_ref[:, e * 128 : (e + 1) * 128] = in_ref[e]
    for s in range(sources):
        input_ref[s * slots : (s + 1) * slots, 0:128] = arrived_ref[s, 0:slots, :]
    input_ref[:, 128:256] = code_ref[...]
    chunk = 256

    def step(c, carry):
        at = pl.multiple_of(c * chunk, chunk)
        inputs = input_ref[pl.ds(at, chunk), :]
        hidden = wide_ref[pl.ds(at, chunk), :]
        stale = stale_ref[pl.ds(at, chunk), :]
        reset = jax.nn.sigmoid(
            matmul(inputs, wx_ref[0]) + matmul(hidden, wh_ref[0]) + bias_ref[0:1, :]
        )
        update = jax.nn.sigmoid(
            matmul(inputs, wx_ref[1]) + matmul(hidden, wh_ref[1]) + bias_ref[1:2, :]
        )
        recall = matmul(hidden, wh_ref[2]) + bias_ref[3:4, :]
        cand = jnp.tanh(matmul(inputs, wx_ref[2]) + bias_ref[2:3, :] + reset * recall)
        fresh = (1.0 - update) * cand + update * stale
        line = lax.broadcasted_iota(I32, (slots, 128), 0).astype(F32)
        live = jnp.concatenate(
            [
                jnp.where(
                    line
                    < arrived_ref[c * (chunk // slots) + k, slots + 8 : slots + 16, :].astype(F32)[
                        3:4
                    ],
                    1.0,
                    0.0,
                )
                for k in range(chunk // slots)
            ],
            axis=0,
        )
        fresh_ref[pl.ds(at, chunk), :] = jnp.where(live > 0.5, fresh, stale)
        reset_ref[pl.ds(at, chunk), :] = reset
        update_ref[pl.ds(at, chunk), :] = update
        recall_ref[pl.ds(at, chunk), :] = recall
        cand_ref[pl.ds(at, chunk), :] = cand
        return carry

    lax.fori_loop(0, stale_ref.shape[0] // chunk, step, 0)


def gates_body(
    grad_ref,
    input_ref,
    wide_ref,
    stale_ref,
    reset_ref,
    update_ref,
    recall_ref,
    cand_ref,
    out_ref,
):
    grad = grad_ref[...]
    reset, update = reset_ref[...], update_ref[...]
    recall, cand = recall_ref[...], cand_ref[...]
    cand_term = grad * (1.0 - update) * (1.0 - cand * cand)
    update_term = grad * (stale_ref[...] - cand) * update * (1.0 - update)
    recall_term = cand_term * reset
    reset_term = cand_term * recall * reset * (1.0 - reset)
    terms = [reset_term, update_term, cand_term, recall_term]
    rounded = [term.astype(BF) for term in terms]
    seen = input_ref.shape[1]
    known = wide_ref.shape[1]
    left = jnp.concatenate(rounded[0:3], axis=1)
    right = jnp.concatenate([rounded[0], rounded[1], rounded[3]], axis=1)
    from_input = matmul_left(input_ref[...], left).astype(BF)
    from_wide = matmul_left(wide_ref[...], right).astype(BF)
    for g in range(3):
        lanes = slice(g * 128, (g + 1) * 128)
        out_ref[g * seen : (g + 1) * seen, :] = from_input[:, lanes]
        out_ref[3 * seen + g * known : 3 * seen + (g + 1) * known, :] = from_wide[:, lanes]
    first = 3 * (seen + known)
    sums = jnp.concatenate(
        [jnp.sum(term, axis=0, keepdims=True) for term in terms] + [jnp.zeros((12, 128), F32)],
        axis=0,
    )
    out_ref[first : first + 16, :] = sums.astype(BF)
    out_ref[first + 16 :, :] = jnp.zeros((out_ref.shape[0] - first - 16, 128), BF)


def weights_body(
    count,
    place_ref,
    wide_ref,
    code_ref,
    mix_ref,
    cot_ref,
    kg_ref,
    vg_ref,
    qg_ref,
    out0_ref,
    out1_ref,
    out2_ref,
    out3_ref,
    block_ref,
):
    place = place_ref[0]
    width = cot_ref.shape[1]
    nodes = cot_ref.shape[0]

    def keep(first, value):
        for e in range(4):
            block_ref[e, first : first + value.shape[0], :] = value[
                :, e * 128 : (e + 1) * 128
            ].astype(BF)

    rows = wide_ref[...]
    keep(0, matmul_left(rows[0:nodes, :], qg_ref[...]))
    keep(width, matmul_left(rows, kg_ref[0:count, :]))
    keep(2 * width, matmul_left(rows, vg_ref[0:count, :]))
    keep(3 * width, matmul_left(code_ref[...], kg_ref[0:count, :]))
    keep(3 * width + 128, matmul_left(mix_ref[...], cot_ref[...]))
    for step, out_ref in enumerate((out0_ref, out1_ref, out2_ref, out3_ref)):
        out_ref[...] = block_ref[(place + step) % 4]


def spread_body(
    place_ref, own_ref, other_ref, query_ref, key_ref, value_ref, time_ref, out_ref, block_ref
):
    emb, core, y, z = (place_ref[k] for k in range(4))
    rows = own_ref.shape[1]

    def put(i, carry):
        e = (emb + 4 - i % 4) % 4
        line = ((z + 4 - (i // 4) % 4) % 4) * 8 + ((y + 4 - i // 16) % 4) * 2
        for ref, c in ((own_ref, core), (other_ref, 1 - core)):
            at = pl.multiple_of((line + c) * rows, 8)
            block_ref[e, pl.ds(at, rows), :] = ref[i].astype(F32)
        return carry

    lax.fori_loop(0, 64, put, 0, unroll=8)
    first = 0
    for ref in (query_ref, key_ref, value_ref, time_ref, out_ref):
        start = first

        def copy(k, carry):
            at = pl.multiple_of(k * 128, 128)
            for e in range(4):
                ref[pl.ds(at, 128), e * 128 : (e + 1) * 128] = block_ref[
                    e, pl.ds(start + at, 128), :
                ]
            return carry

        lax.fori_loop(0, ref.shape[0] // 128, copy, 0, unroll=min(2, ref.shape[0] // 128))
        first += ref.shape[0]


def exchange(value, axes):
    return lax.all_to_all(value, axes, split_axis=0, concat_axis=0, tiled=True)


def fold_body(parts_ref, out_ref):
    count = parts_ref.shape[0]
    total = parts_ref[0].astype(F32)
    for m in range(1, count):
        total = total + parts_ref[m].astype(F32)
    total = total.astype(BF)
    for m in range(count):
        out_ref[m] = total


def fold_one_body(parts_ref, out_ref):
    total = parts_ref[0].astype(F32)
    for m in range(1, parts_ref.shape[0]):
        total = total + parts_ref[m].astype(F32)
    out_ref[0] = total.astype(BF)


def send_mem(value, z_step, y_step, flip):
    pairs = []
    for z in range(4):
        for y in range(4):
            for c in range(2):
                target = ((z + z_step) % 4) * 8 + ((y + y_step) % 4) * 2 + (c ^ flip)
                pairs.append((z * 8 + y * 2 + c, target))
    return lax.ppermute(value, "mem", pairs)


def total_body(own_ref, near_ref, far_ref, last_ref, out_ref):
    rows = own_ref.shape[0]
    total = own_ref[...].astype(F32)
    for ref in (near_ref, far_ref, last_ref):
        total = total + ref[...].astype(F32)
    out_ref[0:rows, :] = total.astype(BF)
    out_ref[rows:, :] = jnp.zeros((out_ref.shape[0] - rows, 128), BF)


def split_body(rows_ref, wx_ref, wh_ref, bias_ref):
    first = 0
    for ref in (wx_ref, wh_ref):
        for g in range(3):
            rows = ref.shape[1]
            ref[g] = rows_ref[first : first + rows, :].astype(F32)
            first += rows
    bias_ref[...] = rows_ref[first : first + 16, :].astype(F32)[0:4]


def reduce_mem(value, count):
    parts = value.reshape(count, value.shape[0] // count, value.shape[1])
    arrived = exchange(parts, "mem")
    folded = call(fold_body, shape(*parts.shape, dtype=BF), (arrived,))
    gathered = exchange(folded, "mem")
    return gathered.reshape(value.shape)


def per_device(
    memory,
    ev_rows,
    ev_count,
    ev_feat,
    ev_dt,
    req_rows,
    nbr_slot,
    nbr_dt,
    nbr_len,
    time_freq,
    gru_wx,
    gru_wh,
    gru_bias,
    w_query,
    w_key,
    w_value,
    w_time,
    w_out,
    cotangent,
):
    columns = memory.shape[1]
    rows_dev = memory.shape[0]
    owners, slot_count = ev_rows.shape[1], ev_rows.shape[2]
    capacity = req_rows.shape[2]
    batch, keys = nbr_slot.shape
    nodes = nbr_len.shape[0]
    peers = batch // nodes
    width = columns * peers
    flat_slots = 640
    table_rows = capacity + 8
    picks = keys * nodes

    packed = call(
        pack_body,
        shape(owners, slot_count + 16, 128, dtype=BF),
        (ev_feat[0], req_rows[0], jnp.transpose(nbr_slot), ev_rows[0], ev_dt[0], ev_count),
        [pltpu.VMEM((owners, flat_slots), I32)],
    )
    arrived = exchange(packed, "mem")

    line = arrived[:, slot_count + 10, :].astype(I32)
    targets = (line[:, :slot_count] * 64 + line[:, slot_count : 2 * slot_count]).reshape(-1)
    deltas = line[:, 2 * slot_count : 3 * slot_count] * 32 + line[:, 3 * slot_count :]
    live_counts = arrived[:, slot_count + 11, 0:1].astype(I32)
    live_mask = (jnp.arange(slot_count, dtype=I32)[None, :] < live_counts).reshape(-1)
    asked = (
        arrived[:, slot_count : slot_count + 5, :].astype(I32) * 64
        + arrived[:, slot_count + 5 : slot_count + 10, :].astype(I32)
    ).reshape(owners, flat_slots)
    asked = jnp.minimum(asked[:, :table_rows], rows_dev - 1)

    place = lax.axis_index("emb").astype(I32).reshape(1)
    total_events = owners * slot_count
    stale_rows, stale_half = call(
        stale_body,
        (shape(total_events, columns), shape(total_events, columns, dtype=BF)),
        (targets, memory),
        scalars=1,
    )
    wide_parts = [stale_half] + [send(stale_half, step, peers) for step in (1, 2, 3)]
    codes_event = time_code(deltas.reshape(-1), time_freq)
    codes, events, ranks = call(
        functools.partial(route_body, slot_count),
        (
            jax.ShapeDtypeStruct((owners, flat_slots), F32),
            jax.ShapeDtypeStruct((owners, flat_slots), F32),
            jax.ShapeDtypeStruct((owners, flat_slots), F32),
        ),
        (arrived,),
        [pltpu.VMEM((owners, flat_slots), F32)],
    )
    index = call(compact_body, shape(8, owners // 8 * BUCKET), (events, ranks))
    fresh_rows, reset, update, recall, cand, inputs, hidden_wide = call(
        cell_body,
        (shape(total_events, columns),) * 5
        + (shape(total_events, 256, dtype=BF), shape(total_events, width, dtype=BF)),
        (place, arrived, codes_event, stale_rows, *wide_parts, gru_wx, gru_wh, gru_bias),
        [pltpu.VMEM((peers, total_events, columns), BF)],
        scalars=1,
    )
    new_memory, outgoing = call(
        refresh_body,
        (shape(rows_dev, columns), shape(owners, table_rows, columns, dtype=BF)),
        (
            targets,
            asked.reshape(-1),
            memory,
            fresh_rows,
            codes,
        ),
        scalars=2,
    )
    fetched = exchange(outgoing, "mem")

    ordered = jnp.transpose(nbr_slot.reshape(peers, nodes, keys), (0, 2, 1)).reshape(peers, -1)
    count = keys * nodes
    row_index = jnp.pad(ordered + 8 * (ordered // capacity), ((0, 0), (0, picks - count)))
    table = fetched.reshape(-1, columns)
    part = shape(picks, columns, dtype=BF)
    row_index = row_index.reshape(-1)

    def taken(steps, extra=()):
        return call(
            functools.partial(take_body, steps, owners),
            (part,) * len(steps) + extra,
            (place, row_index, table),
            [pltpu.VMEM(table.shape, F32)],
            scalars=2,
        )

    near, far, slot_codes = taken((1, 2), (shape(owners, flat_slots),))
    near = send(near, 1, peers)
    far = send(far, 2, peers)
    last, own = taken((3, 0))
    last = send(last, 3, peers)

    slots_in = jnp.pad(ordered, ((0, 0), (0, 24 * 128 - count)), constant_values=-1)
    slots_in = slots_in.reshape(peers, 24, 128)
    pick_rank, slot_list, flag = call(
        functools.partial(picks_body, capacity),
        (
            jax.ShapeDtypeStruct((peers, 24, 128), F32),
            jax.ShapeDtypeStruct((peers, ROWCAP), F32),
            jax.ShapeDtypeStruct((8, 128), F32),
        ),
        (slot_codes, slots_in),
        [pltpu.VMEM((peers, 24, 128), F32)],
    )

    lengths = jnp.broadcast_to(nbr_len.astype(F32)[:, None], (nodes, 128))
    codes_in = time_code(jnp.transpose(nbr_dt).reshape(-1), time_freq)
    padded = 2304
    embedding, mixed, key_grad, value_grad, query_grad, rows_wide, *compact_rows = call(
        functools.partial(attend_body, keys),
        (
            jax.ShapeDtypeStruct((nodes, width), BF),
            jax.ShapeDtypeStruct((nodes, width), BF),
            jax.ShapeDtypeStruct((padded, width), BF),
            jax.ShapeDtypeStruct((padded, width), BF),
            jax.ShapeDtypeStruct((nodes, width), BF),
            jax.ShapeDtypeStruct((count, width), BF),
        )
        + (shape(ROWCAP, columns, dtype=BF),) * 4,
        (
            place,
            own,
            near,
            far,
            last,
            codes_in,
            lengths,
            cotangent,
            pick_rank,
            w_query,
            w_key,
            w_value,
            w_time,
            w_out,
        ),
        [
            pltpu.VMEM((count, width), BF),
            pltpu.VMEM((count, width), BF),
            pltpu.VMEM((nodes, width), F32),
            pltpu.VMEM((nodes, width), F32),
            pltpu.VMEM((nodes, 256), F32),
            pltpu.VMEM((count, 256), F32),
            pltpu.VMEM((count, 256), F32),
            pltpu.VMEM((count, 256), F32),
            pltpu.VMEM((count, 256), F32),
            pltpu.VMEM((nodes, 256), F32),
            pltpu.VMEM((nodes, 256), F32),
            pltpu.VMEM((nodes, width), F32),
            pltpu.VMEM((nodes, width), F32),
            pltpu.VMEM((peers, count, columns), BF),
            pltpu.VMEM((peers, ROWCAP, columns), BF),
        ],
        scalars=1,
        flops=8 * 10**9,
    )

    returned_rows = compact_rows[:1]
    for step in (1, 2, 3):
        returned_rows.append(send(compact_rows[step], step, peers))
    slot_sums = call(
        slots_body,
        shape(owners, BUCKET + 8, columns, dtype=BF),
        (place, slot_list, *returned_rows, flag),
        scalars=1,
    )
    returned = exchange(slot_sums, "mem")
    sparse_grad, flags = call(
        events_body, (shape(total_events, columns), shape(8, 128)), (index, returned)
    )
    spilled = flags[0, 0] > 0.0

    def dense_grad(_):
        key_rows, value_rows = key_grad[:count], value_grad[:count]
        grad = matmul_right(key_rows, w_key) + matmul_right(value_rows, w_value)
        own = matmul_right(query_grad, w_query) + cotangent.astype(F32)
        grad = grad.at[:nodes].add(own).astype(BF)
        parts = jnp.transpose(grad.reshape(count, peers, columns), (1, 0, 2))
        parts = exchange(parts, "emb").reshape(-1, columns).astype(F32)
        sums = call(
            add_rows_body,
            shape(owners * capacity, columns),
            (ordered.reshape(-1), parts),
            scalars=1,
        )
        back = exchange(sums.astype(BF).reshape(owners, capacity, columns), "mem")
        table = call(
            add_rows_body,
            shape(rows_dev, columns),
            (asked[:, :capacity].reshape(-1), back.reshape(-1, columns).astype(F32)),
            scalars=1,
        )
        return jnp.where(live_mask[:, None], table[targets], 0.0)

    grad_fresh = lax.cond(spilled, dense_grad, lambda kept: kept, sparse_grad)

    total_weight = 3 * width + 128 + width
    shard = owners * 80
    weight_parts = call(
        functools.partial(weights_body, count),
        (shape(total_weight, columns, dtype=BF),) * 4,
        (
            place,
            rows_wide,
            codes_in,
            mixed,
            cotangent,
            key_grad,
            value_grad,
            query_grad,
        ),
        [pltpu.VMEM((peers, total_weight, columns), BF)],
        scalars=1,
        flops=2 * 10**9,
    )
    moved = [weight_parts[0]]
    for step in (1, 2, 3):
        moved.append(send(weight_parts[step], step, peers))
    weight_sum = call(total_body, shape(owners * 72, columns, dtype=BF), tuple(moved))
    arrived_parts = exchange(weight_sum.reshape(owners, 72, columns), "mem")
    ring = call(fold_one_body, shape(1, 72, columns, dtype=BF), (arrived_parts,))
    ring = jnp.concatenate([ring] + [send(ring, d, peers) for d in (1, 2, 3)], axis=0)
    ring = jnp.concatenate([ring] + [send_mem(ring, d, 0, 0) for d in (1, 2, 3)], axis=0)
    ring = jnp.concatenate([ring] + [send_mem(ring, 0, d, 0) for d in (1, 2, 3)], axis=0)
    other = send_mem(ring, 0, 0, 1)
    mem = lax.axis_index("mem").astype(I32)
    corner = jnp.stack([place[0], mem % 2, (mem // 2) % 4, mem // 8])
    grad_query, grad_key, grad_value, grad_time, grad_out = call(
        spread_body,
        (
            shape(width, width),
            shape(width, width),
            shape(width, width),
            shape(128, width),
            shape(width, width),
        ),
        (corner, ring, other),
        [pltpu.VMEM((peers, owners * 72, columns), F32)],
        scalars=1,
    )

    gate_rows = call(
        gates_body,
        shape(shard, columns, dtype=BF),
        (grad_fresh, inputs, hidden_wide, stale_rows, reset, update, recall, cand),
    )
    gate_rows = reduce_mem(gate_rows, owners)
    grad_wx, grad_wh, grad_bias = call(
        split_body,
        (shape(*gru_wx.shape), shape(*gru_wh.shape), shape(*gru_bias.shape)),
        (gate_rows,),
    )
    return (
        new_memory,
        embedding,
        grad_wx,
        grad_wh,
        grad_bias,
        grad_query,
        grad_key,
        grad_value,
        grad_time,
        grad_out,
    )


def solution(mesh):
    in_specs = (
        P("mem", "emb"),
        P("mem", None, None),
        P("mem", None),
        P("mem", None, None, None),
        P("mem", None, None),
        P("mem", None, None),
        P("mem", None),
        P(("mem", "emb"), None),
        P(("mem", "emb")),
        P(),
        P(None, None, "emb"),
        P(None, None, "emb"),
        P(None, "emb"),
        P(),
        P(),
        P(),
        P(),
        P(),
        P(("mem", "emb"), None),
    )
    out_specs = (
        P("mem", "emb"),
        P(("mem", "emb"), None),
        P(None, None, "emb"),
        P(None, None, "emb"),
        P(None, "emb"),
        P(),
        P(),
        P(),
        P(),
        P(),
    )

    return jax.shard_map(
        per_device, mesh=mesh, in_specs=in_specs, out_specs=out_specs, check_vma=False
    )
```
